32 devices in a mesh: segment: 4 (over y, x), gy: 8 (over z, core).
Axes of the slice: x: 2, y: 2, z: 4, core: 2. Of those that a mesh axis runs over, the one named last changes fastest.
Arguments:
- crops: bfloat16 [2, 32, 4, 32, 128], P(None, None, None, 'gy'), may hold values from -6 to 6
- cotangent: bfloat16 [2, 32, 4, 32, 128], P(None, None, None, 'gy'), may hold values from -0.59765625 to 0.59765625
- weights: bfloat16 [4, 2, 27, 32, 32], P('segment'), may hold values from -0.375 to 0.375
Outputs:
- features: bfloat16 [4, 2, 32, 4, 32, 128], P('segment', None, None, None, 'gy')
- weight_grads: float32 [4, 2, 27, 32, 32], P('segment')
- input_grads: float32 [4, 2, 32, 4, 32, 128], P('segment', None, None, None, 'gy')
The draws below stay inside these ranges and needn't reach their ends.
All inputs are finite; a program needn't handle non-finite values.
Results may differ from the reference program's by a relative error of at most 0.025.
Values may be sent and summed in bfloat16 or wider, within the bound.
A program may use at most 128 MiB of HBM per device.

```python
import jax
import jax.numpy as jnp
from jax import lax

C = 32
MICRO = 2
Z = 4
X = 128
Y = 32


def steps_of(rng, dims, split, smallest, high):
    def one(dim, shards_of):
        steps = jax.random.uniform(jax.random.fold_in(jax.random.fold_in(rng, 6), dim), (shards_of,), jnp.float32, smallest / len(split), high / len(split))
        return jnp.repeat(jnp.exp(steps), dims[dim] // shards_of).reshape((-1,) + (1,) * (len(dims) - dim - 1))

    factor_of = one(*split[0])
    for cut in split[1:]:
        factor_of = factor_of * one(*cut)
    return factor_of


def gaussian(rng, shape, scale, most, split=(), held_as=jnp.bfloat16):
    gain = steps_of(rng, shape, split, -0.22, 0.18) if split else 1.0
    drawn = jax.random.normal(rng, shape, jnp.float32) * scale * gain
    return jnp.minimum(jnp.maximum(drawn, -most), most).astype(held_as)


def setup_inputs(seed: int = 0) -> dict:
    key_of = jax.random.split(jax.random.key(seed), 4)
    crops = gaussian(key_of[0], (MICRO, C, Z, Y, X), 1.0, 6.0, ((3, 8),))
    cotangent = gaussian(key_of[1], (MICRO, C, Z, Y, X), 0.1, 0.59765625, ((3, 8),))
    weights = gaussian(key_of[2], (4, 2, 27, C, C), (9 * C) ** -0.5, 0.375, ((0, 4),))
    return {"crops": crops, "cotangent": cotangent, "weights": weights}


def surround(volume):
    return jnp.pad(volume, ((0, 0), (1, 1), (1, 1), (1, 1)))


def slices_of(padded, plane_shift, row_count):
    planes = padded.shape[1] - 2
    across = padded.shape[3] - 2
    return jnp.stack([padded[:, plane_shift:plane_shift + planes, row_shift:row_shift + row_count, side_shift:side_shift + across] for row_shift in range(3) for side_shift in range(3)])


def convolve(padded, kernel, row_count):
    result = None
    for plane_shift in range(3):
        stacked = slices_of(padded, plane_shift, row_count).astype(jnp.float32)
        tap_weights = kernel[9 * plane_shift:9 * plane_shift + 9].astype(jnp.float32)
        contribution = jnp.einsum("tczyx,tco->ozyx", stacked, tap_weights, precision=lax.Precision.HIGHEST)
        result = contribution if result is None else result + contribution
    return result


def kernel_grads(padded, gradient, row_count):
    pieces = []
    for plane_shift in range(3):
        stacked = slices_of(padded, plane_shift, row_count).astype(jnp.float32)
        pieces.append(jnp.einsum("tczyx,ozyx->tco", stacked, gradient.astype(jnp.float32), precision=lax.Precision.HIGHEST))
    return jnp.concatenate(pieces, 0)


def flipped(kernel):
    return jnp.transpose(jnp.flip(kernel, 0), (0, 2, 1))


def slope(preact):
    logistic = jax.nn.sigmoid(preact)
    return logistic * (1.0 + preact * (1.0 - logistic))


def reference(crops, cotangent, weights):
    row_count = crops.shape[3]
    features = []
    input_grads = []
    weight_grads = jnp.zeros(weights.shape, jnp.float32)
    for micro_index in range(MICRO):
        entries = []
        stored = []
        carried = crops[micro_index]
        for section in range(4):
            entering = carried
            entries.append(entering)
            if section >= 2:
                merged = (entering.astype(jnp.float32) + entries[3 - section].astype(jnp.float32)).astype(jnp.bfloat16)
            else:
                merged = entering
            input_pad = surround(merged)
            pre_first = convolve(input_pad, weights[section, 0], row_count)
            hidden_pad = surround(jax.nn.silu(pre_first).astype(jnp.bfloat16))
            pre_second = convolve(hidden_pad, weights[section, 1], row_count)
            carried = jax.nn.silu(pre_second).astype(jnp.bfloat16)
            stored.append((input_pad, pre_first, hidden_pad, pre_second, carried))
        incoming = cotangent[micro_index]
        deltas = [None, None, None, None]
        sums = [None, None, None, None]
        for section in (3, 2, 1, 0):
            input_pad, pre_first, hidden_pad, pre_second, unused_out = stored[section]
            second_delta = (incoming.astype(jnp.float32) * slope(pre_second)).astype(jnp.bfloat16)
            grad_second = kernel_grads(hidden_pad, second_delta, row_count)
            hidden_delta = convolve(surround(second_delta), flipped(weights[section, 1]), row_count)
            first_delta = (hidden_delta * slope(pre_first)).astype(jnp.bfloat16)
            grad_first = kernel_grads(input_pad, first_delta, row_count)
            weight_grads = weight_grads.at[section].add(jnp.stack([grad_first, grad_second]))
            deltas[section] = convolve(surround(first_delta), flipped(weights[section, 0]), row_count).astype(jnp.bfloat16)
            if section == 1:
                sums[1] = deltas[1].astype(jnp.float32) + deltas[2].astype(jnp.float32)
                incoming = sums[1].astype(jnp.bfloat16)
            elif section == 0:
                sums[0] = deltas[0].astype(jnp.float32) + deltas[3].astype(jnp.float32)
            else:
                sums[section] = deltas[section].astype(jnp.float32)
                incoming = deltas[section]
        input_grads.append(jnp.stack(sums))
        features.append(jnp.stack([stored[section][4] for section in range(4)]))
    return jnp.stack(features, 1), weight_grads, jnp.stack(input_grads, 1)
```

```python
import functools

import jax
import jax.numpy as jnp
from jax import lax
from jax.experimental import pallas as pl
from jax.experimental.pallas import tpu as pltpu
from jax.sharding import PartitionSpec as P

HALO = 2
CHUNKS = 32
MESH = pl.DeviceIdType.MESH


def logistic_of(value):
    return 0.5 + 0.5 * jnp.tanh(0.5 * value)


def shifted(value, by):
    across = value.shape[-1]
    lane = lax.broadcasted_iota(jnp.int32, value.shape, value.ndim - 1)
    if by == 1:
        return jnp.where(lane == 0, 0.0, pltpu.roll(value, 1, value.ndim - 1))
    return jnp.where(lane == across - 1, 0.0, pltpu.roll(value, across - 1, value.ndim - 1))


def network_kernel(
    sizes,
    sections,
    count,
    crop_ref,
    cot_ref,
    own_ref,
    feat_out,
    grad_out,
    wg_out,
    frame,
    hidden,
    sdelta,
    fdelta,
    slope1,
    slope2,
    feats,
    grads,
    halo,
    wbuf,
    taps,
    shifts,
    part,
    gathered,
    reduced,
    halo_send,
    halo_recv,
    w_send,
    w_recv,
    f_send,
    f_recv,
    out_send,
    out_recv,
    rs_send,
    rs_recv,
    ag_send,
    ag_recv,
):
    channels, planes, rows, across = sizes
    inner = rows + 2
    seg = lax.axis_index("segment")
    gy = lax.axis_index("gy")
    micro = seg % 2
    upper = seg // 2
    core = gy % 2
    sibling = gy + 1 - 2 * core
    partner = seg + 1 - 2 * micro
    top, bottom = HALO * channels, (HALO + rows) * channels
    has_low, has_high = gy > 0, gy < count - 1
    own_chunks = CHUNKS // count

    barrier = pltpu.get_barrier_semaphore()

    def greet(s, g):
        pl.semaphore_signal(barrier, inc=1, device_id=(s, g), device_id_type=MESH)

    for d in range(1, count):
        greet(seg, (gy + d) % count)
    for d in range(count):
        greet(partner, (gy + d) % count)
    greet((seg + 2) % sections, gy)
    greet((partner + 2) % sections, gy)

    zero_half = jnp.zeros((frame.shape[-2], across), jnp.bfloat16)
    zero_row = jnp.zeros((channels, 2 * across), jnp.bfloat16)
    for group in (frame, hidden, sdelta, fdelta):
        for s in range(group.shape[0]):
            group[s, 0, :, :across] = zero_half
            group[s, planes, :, across:] = zero_half
    for group in (hidden, fdelta):
        for s in range(group.shape[0]):
            for p in range(planes + 1):
                group[s, p, :channels] = zero_row
                group[s, p, (inner + 1) * channels :] = zero_row
    def blank(side):
        halo[:, side] = jnp.zeros(halo.shape[:1] + halo.shape[2:], jnp.bfloat16)

    pl.when(gy == 0)(lambda: blank(0))
    pl.when(gy == count - 1)(lambda: blank(1))
    part[...] = jnp.zeros(part.shape, jnp.bfloat16)
    wbuf[seg] = own_ref[...]

    def put(group, s, z, low, value):
        high = low + value.shape[0]
        group[s, z + 1, low:high, :across] = value
        group[s, z, low:high, across:] = value

    for z in range(planes):
        put(frame, 0, z, top, crop_ref[z])

    pl.semaphore_wait(barrier, 2 * count - 1 + 2)

    def halo_copy(group, s, stage, side):
        low = top if side == 1 else bottom - HALO * channels
        target = gy - 1 if side == 1 else gy + 1
        return pltpu.make_async_remote_copy(
            src_ref=group.at[s, pl.ds(1, planes), pl.ds(low, HALO * channels), pl.ds(0, across)],
            dst_ref=halo.at[stage, side],
            send_sem=halo_send.at[stage, side],
            recv_sem=halo_recv.at[stage, side],
            device_id=(seg, target),
            device_id_type=MESH,
        )

    def start_halo(group, s, stage):
        @pl.when(has_low)
        def _():
            halo_copy(group, s, stage, 1).start()

        @pl.when(has_high)
        def _():
            halo_copy(group, s, stage, 0).start()

    def finish_halo(group, s, stage):
        @pl.when(has_low)
        def _():
            halo_copy(group, s, stage, 0).wait_recv()

        @pl.when(has_high)
        def _():
            halo_copy(group, s, stage, 1).wait_recv()

        for z in range(planes):
            put(group, s, z, 0, halo[stage, 0, z])
            put(group, s, z, bottom, halo[stage, 1, z])

    def drain_halo(group, s, stage):
        @pl.when(has_low)
        def _():
            halo_copy(group, s, stage, 1).wait_send()

        @pl.when(has_high)
        def _():
            halo_copy(group, s, stage, 0).wait_send()

    def weight_copy(step, direction):
        return pltpu.make_async_remote_copy(
            src_ref=own_ref.at[direction, core],
            dst_ref=wbuf.at[seg, direction, core],
            send_sem=w_send.at[step - 1, direction],
            recv_sem=w_recv.at[step - 1, direction],
            device_id=((seg + step) % sections, gy),
            device_id_type=MESH,
        )

    def forward_copy(step, direction):
        where = wbuf.at[(seg - step + sections) % sections, direction, core]
        return pltpu.make_async_remote_copy(
            src_ref=where,
            dst_ref=where,
            send_sem=f_send.at[step - 1, direction],
            recv_sem=f_recv.at[step - 1, direction],
            device_id=(seg, sibling),
            device_id_type=MESH,
        )

    start_halo(frame, 0, 0)
    for direction in range(2):
        for step in range(1, sections):
            weight_copy(step, direction).start()

    def pass_on(s, direction):
        step = (seg - s + sections) % sections

        @pl.when(step > 0)
        def _():
            weight_copy(step, direction).wait_recv()
            forward_copy(step, direction).start()

    def arrived(s, direction):
        step = (seg - s + sections) % sections

        @pl.when(step > 0)
        def _():
            forward_copy(step, direction).wait_recv()

    def build(s, direction, conv):
        into = taps.at[s, direction, conv]
        for dz in range(3):
            for dx in range(3):
                compact = wbuf[s, direction, conv, 3 * dz + dx].astype(jnp.float32)
                wide = jnp.concatenate([compact, jnp.zeros_like(compact)], 1)
                for y in range(inner):
                    moved = wide if y == 0 else pltpu.roll(wide, y * channels, 1)
                    row = (3 * y + dx) * channels
                    into[row : row + channels, dz * 2 * across : (dz + 1) * 2 * across] = (
                        moved.astype(jnp.bfloat16)
                    )

    def convolve(s, direction, conv, group, index, pair, low, high):
        matrix = taps[s, direction, conv, 3 * low * channels : 3 * high * channels, :]
        span = group.shape[-2]
        stacked = group[index, 2 * pair : 2 * pair + 3].reshape(3 * span, 2 * across)
        full = jnp.dot(matrix, stacked, preferred_element_type=jnp.float32)
        full = full.reshape(high - low, 3, channels, 2 * across)
        halves = []
        for half in range(2):
            a, b, c = (
                full[:, dx, :, half * across : (half + 1) * across].reshape(
                    (high - low) * channels, across
                )
                for dx in range(3)
            )
            halves.append(shifted(a, 1) + b + shifted(c, -1))
        return halves

    frame_row = lax.broadcasted_iota(jnp.int32, (inner * channels, across), 0) // channels + 1
    inside_low = jnp.where(gy == 0, HALO, 0)
    inside_high = jnp.where(gy == count - 1, rows + HALO, rows + 2 * HALO)
    mask = (frame_row >= inside_low) & (frame_row < inside_high)

    def weight_terms(slot, conv, group, s, delta_group, index):
        for z in range(planes):
            delta = delta_group[index, z + 1, top:bottom, :across].astype(jnp.float32)
            for dx, field in enumerate((shifted(delta, -1), delta, shifted(delta, 1))):
                shifts[
                    z // 2,
                    dx * rows * channels : (dx + 1) * rows * channels,
                    (z % 2) * across : (z % 2 + 1) * across,
                ] = field.astype(jnp.bfloat16)
        lane = lax.broadcasted_iota(jnp.int32, (channels, across), 1) // channels
        fields = []
        for dz in range(3):
            total = None
            for pair in range(planes // 2):
                term = lax.dot_general(
                    group[s, 2 * pair + dz, channels : (inner + 1) * channels, :],
                    shifts[pair],
                    (((1,), (1,)), ((), ())),
                    preferred_element_type=jnp.float32,
                )
                total = term if total is None else total + term
            for dy in range(3):
                for dx in range(3):
                    picked = None
                    for y in range(rows):
                        block = total[
                            (y + dy) * channels : (y + dy + 1) * channels,
                            dx * rows * channels : (dx + 1) * rows * channels,
                        ]
                        picked = block if picked is None else jnp.where(lane == y, block, picked)
                    fields.append(picked)
        fields.append(jnp.zeros((channels, across), jnp.float32))
        first_half = lane < 2
        even = lane % 2 == 0
        half = across // 2
        for k in range(7):
            r = fields[4 * k : 4 * k + 4]
            pairs = [
                jnp.where(first_half, r[i], r[i + 2])
                + pltpu.roll(jnp.where(first_half, r[i + 2], r[i]), half, 1)
                for i in range(2)
            ]
            packed = jnp.where(
                even,
                pairs[0] + pltpu.roll(pairs[0], across - channels, 1),
                pairs[1] + pltpu.roll(pairs[1], channels, 1),
            ).astype(jnp.bfloat16)
            for piece in range(2):
                part[slot, 16 * conv + 2 * k + piece] = packed[16 * piece : 16 * piece + 16]

    def out_copy(source, into, kind):
        return pltpu.make_async_remote_copy(
            src_ref=source.at[partner],
            dst_ref=into.at[micro],
            send_sem=out_send.at[kind],
            recv_sem=out_recv.at[kind],
            device_id=(partner, gy),
            device_id_type=MESH,
        )

    pass_on(0, 0)
    arrived(0, 0)
    build(0, 0, 0)
    build(0, 0, 1)
    for s in range(sections):
        if s + 1 < sections:
            pass_on(s + 1, 0)
        finish_halo(frame, s, s)
        for pair in range(planes // 2):
            for half, pre in enumerate(convolve(s, 0, 0, frame, s, pair, 0, inner)):
                z = 2 * pair + half
                logistic = logistic_of(pre)
                slope1[s, z] = logistic * (1.0 + pre * (1.0 - logistic))
                put(
                    hidden, s, z, channels,
                    jnp.where(mask, pre * logistic, 0.0).astype(jnp.bfloat16),
                )
        for pair in range(planes // 2):
            for half, pre in enumerate(convolve(s, 0, 1, hidden, s, pair, 1, rows + 1)):
                z = 2 * pair + half
                logistic = logistic_of(pre)
                slope = logistic * (1.0 + pre * (1.0 - logistic))
                leaving = (pre * logistic).astype(jnp.bfloat16)
                feats[s, z] = leaving
                if s + 1 == sections:
                    second = (cot_ref[z].astype(jnp.float32) * slope).astype(jnp.bfloat16)
                    put(sdelta, s, z, top, second)
                    continue
                slope2[s, z] = slope
                if s in (1, 2):
                    skip = feats[0, z] if s == 1 else crop_ref[z]
                    leaving = (
                        leaving.astype(jnp.float32) + skip.astype(jnp.float32)
                    ).astype(jnp.bfloat16)
                put(frame, s + 1, z, top, leaving)
        if s + 1 < sections:
            start_halo(frame, s + 1, s + 1)
            arrived(s + 1, 0)
            build(s + 1, 0, 0)
            build(s + 1, 0, 1)
        else:
            start_halo(sdelta, s, sections + s)
        pass_on(sections - 1 - s, 1)

    out_copy(feats, feat_out, 0).start()
    feat_out[micro] = feats[seg]
    arrived(sections - 1, 1)
    build(sections - 1, 1, 1)
    build(sections - 1, 1, 0)
    for s in reversed(range(sections)):
        @pl.when(upper == s // 2)
        def _():
            weight_terms(s % 2, 1, hidden, s, sdelta, s)

        finish_halo(sdelta, s, sections + s)
        for pair in range(planes // 2):
            for half, pre in enumerate(convolve(s, 1, 1, sdelta, s, pair, 0, inner)):
                z = 2 * pair + half
                put(
                    fdelta, 0, z, channels,
                    jnp.where(mask, pre * slope1[s, z], 0.0).astype(jnp.bfloat16),
                )
        for pair in range(planes // 2):
            for half, pre in enumerate(convolve(s, 1, 0, fdelta, 0, pair, 1, rows + 1)):
                z = 2 * pair + half
                value = pre.astype(jnp.bfloat16)
                if s < 2:
                    value = (
                        value.astype(jnp.float32) + grads[3 - s, z].astype(jnp.float32)
                    ).astype(jnp.bfloat16)
                grads[s, z] = value
                if s > 0:
                    put(
                        sdelta, s - 1, z, top,
                        (value.astype(jnp.float32) * slope2[s - 1, z]).astype(jnp.bfloat16),
                    )
        if s > 0:
            start_halo(sdelta, s - 1, sections + s - 1)
        else:
            out_copy(grads, grad_out, 1).start()
        @pl.when(upper == s // 2)
        def _():
            weight_terms(s % 2, 0, frame, s, fdelta, 0)

        if s > 0:
            arrived(s - 1, 1)
            build(s - 1, 1, 1)
            build(s - 1, 1, 0)

    me = micro * count + gy

    def share_copy(slot, peer):
        return pltpu.make_async_remote_copy(
            src_ref=part.at[slot, pl.ds(peer * own_chunks, own_chunks)],
            dst_ref=gathered.at[me],
            send_sem=rs_send.at[slot * count + peer],
            recv_sem=rs_recv.at[me],
            device_id=(2 * upper + slot, peer),
            device_id_type=MESH,
        )

    def share_wait(sender):
        return pltpu.make_async_remote_copy(
            src_ref=part.at[0, pl.ds(0, own_chunks)],
            dst_ref=gathered.at[sender],
            send_sem=rs_send.at[0],
            recv_sem=rs_recv.at[sender],
            device_id=(partner, gy),
            device_id_type=MESH,
        )

    targets = [((micro + 1) % 2, gy)]
    for d in range(1, count):
        peer = (gy + d) % count
        targets += [(micro, peer), ((micro + 1) % 2, peer)]
    for slot, peer in targets:
        share_copy(slot, peer).start()
    grad_out[micro] = grads[seg]
    total = part[micro, pl.ds(gy * own_chunks, own_chunks)].astype(jnp.float32)
    for slot, peer in targets:
        sender = slot * count + peer
        share_wait(sender).wait_recv()
        total = total + gathered[sender].astype(jnp.float32)
    reduced[gy] = total.astype(jnp.bfloat16)

    def whole_copy(peer, owner):
        return pltpu.make_async_remote_copy(
            src_ref=reduced.at[owner],
            dst_ref=reduced.at[owner],
            send_sem=ag_send.at[peer],
            recv_sem=ag_recv.at[owner],
            device_id=(seg, peer),
            device_id_type=MESH,
        )

    peers = [(gy + d) % count for d in range(1, count)]
    for peer in peers:
        whole_copy(peer, gy).start()
    for peer in peers:
        whole_copy(peer, peer).wait_recv()
    everything = reduced[...].reshape(CHUNKS, 16, across)
    for conv in range(2):
        for t in range(27):
            k, lane_group = t // 4, t % 4
            for piece in range(2):
                block = everything[16 * conv + 2 * k + piece].astype(jnp.float32)
                if lane_group:
                    block = pltpu.roll(block, across - lane_group * channels, 1)
                wg_out[conv, t, 16 * piece : 16 * piece + 16] = block[:, :channels]

    for kind, (source, into) in enumerate(((feats, feat_out), (grads, grad_out))):
        out_copy(source, into, kind).wait()
    for s in range(sections):
        drain_halo(frame, s, s)
        drain_halo(sdelta, s, sections + s)
    for direction in range(2):
        for step in range(1, sections):
            weight_copy(step, direction).wait_send()
            forward_copy(step, direction).wait_send()
    for slot, peer in targets:
        share_copy(slot, peer).wait_send()
    for peer in peers:
        whole_copy(peer, gy).wait_send()


def local(crops, cotangent, weights):
    micro_count, channels, planes, rows, across = crops.shape
    sizes = (channels, planes, rows, across)
    segment = lax.axis_index("segment")
    sections = lax.axis_size("segment")
    count = lax.axis_size("gy")
    micro = segment % 2
    inner = rows + 2
    span = (rows + 2 * HALO) * channels
    vmem = pl.BlockSpec(memory_space=pltpu.VMEM)
    bf = lambda *shape: pltpu.VMEM(shape, jnp.bfloat16)
    fl = lambda *shape: pltpu.VMEM(shape, jnp.float32)
    dma = lambda *shape: pltpu.SemaphoreType.DMA(shape)

    kernels = weights[0].reshape(2, 3, 3, 3, channels, channels)
    straight = jnp.transpose(kernels, (0, 1, 3, 5, 2, 4))
    turned = jnp.transpose(jnp.flip(kernels, (1, 2, 3)), (0, 1, 3, 4, 2, 5))
    compact = jnp.stack([straight, turned]).reshape(2, 2, 9, channels, 3 * channels)
    compact = jnp.pad(compact, ((0, 0),) * 4 + ((0, 128 - 3 * channels),))

    def arranged(field):
        mine = lax.dynamic_index_in_dim(field, micro, 0, keepdims=False)
        return jnp.transpose(mine, (1, 2, 0, 3)).reshape(planes, rows * channels, across)

    band = (planes, rows * channels, across)
    double = (planes + 1, span, 2 * across)
    chunk = (CHUNKS // count, 16, across)
    features, grads, weight_grads = pl.pallas_call(
        functools.partial(network_kernel, sizes, sections, count),
        out_shape=(
            jax.ShapeDtypeStruct((2, *band), jnp.bfloat16),
            jax.ShapeDtypeStruct((2, *band), jnp.bfloat16),
            jax.ShapeDtypeStruct((2, 27, channels, channels), jnp.float32),
        ),
        in_specs=[vmem] * 3,
        out_specs=(vmem,) * 3,
        scratch_shapes=[
            bf(sections, *double),
            bf(sections, *double),
            bf(sections, *double),
            bf(1, *double),
            fl(sections, planes, inner * channels, across),
            fl(sections, *band),
            bf(sections, *band),
            bf(sections, *band),
            bf(2 * sections, 2, planes, HALO * channels, across),
            bf(sections, 2, 2, 9, channels, across),
            bf(sections, 2, 2, 3 * inner * channels, 3 * span),
            bf(planes // 2, 3 * rows * channels, 2 * across),
            bf(2, CHUNKS, 16, across),
            bf(2 * count, *chunk),
            bf(count, *chunk),
            dma(2 * sections, 2),
            dma(2 * sections, 2),
            dma(sections - 1, 2),
            dma(sections - 1, 2),
            dma(sections - 1, 2),
            dma(sections - 1, 2),
            dma(2),
            dma(2),
            dma(2 * count),
            dma(2 * count),
            dma(count),
            dma(count),
        ],
        compiler_params=pltpu.CompilerParams(
            vmem_limit_bytes=56 * 2**20, collective_id=0, has_side_effects=True
        ),
    )(arranged(crops), arranged(cotangent), compact)

    def restored(field):
        return jnp.transpose(
            field.reshape(2, planes, rows, channels, across), (0, 3, 1, 2, 4)
        )

    return (
        restored(features)[None],
        weight_grads[None],
        restored(grads).astype(jnp.float32)[None],
    )


def solution(mesh):
    return jax.shard_map(
        local,
        mesh=mesh,
        in_specs=(
            P(None, None, None, "gy", None),
            P(None, None, None, "gy", None),
            P("segment", None, None, None, None),
        ),
        out_specs=(
            P("segment", None, None, None, "gy", None),
            P("segment", None, None, None, None),
            P("segment", None, None, None, "gy", None),
        ),
        check_vma=False,
    )
```

```python
import functools

import jax
import jax.numpy as jnp
from jax import lax
from jax.experimental import pallas as pl
from jax.experimental.pallas import tpu as pltpu
from jax.sharding import PartitionSpec as P

HALO = 2
PIECES = 32
PIECE_ROWS = 8
MESH = pl.DeviceIdType.MESH


def logistic_of(value):
    return 0.5 + 0.5 * jnp.tanh(0.5 * value)


def shifted(value, by):
    across = value.shape[-1]
    lane = lax.broadcasted_iota(jnp.int32, value.shape, value.ndim - 1)
    if by == 1:
        return jnp.where(lane == 0, 0.0, pltpu.roll(value, 1, value.ndim - 1))
    return jnp.where(lane == across - 1, 0.0, pltpu.roll(value, across - 1, value.ndim - 1))


def network_kernel(
    sizes,
    sections,
    count,
    crop_hbm,
    cot_hbm,
    own_hbm,
    feat_out,
    grad_out,
    reduced,
    crop_flat,
    cot_flat,
    own_ref,
    crop_ref,
    cot_ref,
    frame,
    hidden,
    sdelta,
    fdelta,
    slope1,
    slope2,
    feats,
    grads,
    halo,
    wbuf,
    taps,
    shifts,
    part,
    gathered,
    in_sem,
    halo_send,
    halo_recv,
    w_send,
    w_recv,
    f_send,
    f_recv,
    out_send,
    out_recv,
    rs_send,
    rs_recv,
    ag_send,
    ag_recv,
):
    channels, planes, rows, across = sizes
    inner = rows + 2
    seg = lax.axis_index("segment")
    gy = lax.axis_index("gy")
    micro = seg % 2
    upper = seg // 2
    core = gy % 2
    sibling = gy + 1 - 2 * core
    partner = seg + 1 - 2 * micro
    top, bottom = HALO * channels, (HALO + rows) * channels
    has_low, has_high = gy > 0, gy < count - 1
    share = PIECES // count

    loads = [
        pltpu.make_async_copy(source, into, in_sem.at[k])
        for k, (source, into) in enumerate(
            (
                (crop_hbm.at[micro], crop_flat),
                (own_hbm, own_ref),
                (cot_hbm.at[micro], cot_flat),
            )
        )
    ]
    for load in loads:
        load.start()

    def blank(side):
        halo[:, side] = jnp.zeros(halo.shape[:1] + halo.shape[2:], jnp.bfloat16)

    pl.when(gy == 0)(lambda: blank(0))
    pl.when(gy == count - 1)(lambda: blank(1))

    barrier = pltpu.get_barrier_semaphore()

    def greet(s, g):
        pl.semaphore_signal(barrier, inc=1, device_id=(s, g), device_id_type=MESH)

    for d in range(1, count):
        greet(seg, (gy + d) % count)
    for d in range(count):
        greet(partner, (gy + d) % count)
    greet((seg + 2) % sections, gy)
    greet((partner + 2) % sections, gy)

    def put(group, s, z, low, value):
        high = low + value.shape[0]
        group[s, z + 1, low:high, :across] = value
        group[s, z, low:high, across:] = value

    def by_plane(flat, z):
        size = (rows * channels, channels * planes * rows)
        place = lax.broadcasted_iota(jnp.int32, size, 0)
        source = lax.broadcasted_iota(jnp.int32, size, 1)
        wanted = (place % channels) * (planes * rows) + z * rows + place // channels
        pick = jnp.where(source == wanted, 1.0, 0.0).astype(jnp.bfloat16)
        return jnp.dot(pick, flat[...], preferred_element_type=jnp.float32).astype(jnp.bfloat16)

    loads[0].wait()
    for z in range(planes):
        plane = by_plane(crop_flat, z)
        crop_ref[z] = plane
        put(frame, 0, z, top, plane)

    pl.semaphore_wait(barrier, 2 * count - 1 + 2)

    def halo_copy(group, s, stage, side):
        low = top if side == 1 else bottom - HALO * channels
        target = gy - 1 if side == 1 else gy + 1
        return pltpu.make_async_remote_copy(
            src_ref=group.at[s, pl.ds(1, planes), pl.ds(low, HALO * channels), pl.ds(0, across)],
            dst_ref=halo.at[stage, side],
            send_sem=halo_send.at[stage, side],
            recv_sem=halo_recv.at[stage, side],
            device_id=(seg, target),
            device_id_type=MESH,
        )

    def start_halo(group, s, stage):
        @pl.when(has_low)
        def _():
            halo_copy(group, s, stage, 1).start()

        @pl.when(has_high)
        def _():
            halo_copy(group, s, stage, 0).start()

    def finish_halo(group, s, stage):
        @pl.when(has_low)
        def _():
            halo_copy(group, s, stage, 0).wait_recv()

        @pl.when(has_high)
        def _():
            halo_copy(group, s, stage, 1).wait_recv()

        for z in range(planes):
            put(group, s, z, 0, halo[stage, 0, z])
            put(group, s, z, bottom, halo[stage, 1, z])

    def drain_halo(group, s, stage):
        @pl.when(has_low)
        def _():
            halo_copy(group, s, stage, 1).wait_send()

        @pl.when(has_high)
        def _():
            halo_copy(group, s, stage, 0).wait_send()

    half_rows = channels // 2

    def weight_copy(step, direction, conv):
        return pltpu.make_async_remote_copy(
            src_ref=wbuf.at[seg, direction, conv, :, pl.ds(core * half_rows, half_rows)],
            dst_ref=wbuf.at[seg, direction, conv, :, pl.ds(core * half_rows, half_rows)],
            send_sem=w_send.at[step - 1, direction, conv],
            recv_sem=w_recv.at[step - 1, direction, conv],
            device_id=((seg + step) % sections, gy),
            device_id_type=MESH,
        )

    def weight_wait(step, direction, conv):
        where = wbuf.at[
            (seg - step + sections) % sections, direction, conv, :,
            pl.ds(core * half_rows, half_rows),
        ]
        return pltpu.make_async_remote_copy(
            src_ref=where,
            dst_ref=where,
            send_sem=w_send.at[step - 1, direction, conv],
            recv_sem=w_recv.at[step - 1, direction, conv],
            device_id=(seg, sibling),
            device_id_type=MESH,
        )

    def forward_copy(step, direction, conv, half=None):
        half = core if half is None else half
        where = wbuf.at[
            (seg - step + sections) % sections, direction, conv, :,
            pl.ds(half * half_rows, half_rows),
        ]
        return pltpu.make_async_remote_copy(
            src_ref=where,
            dst_ref=where,
            send_sem=f_send.at[step - 1, direction, conv],
            recv_sem=f_recv.at[step - 1, direction, conv],
            device_id=(seg, sibling),
            device_id_type=MESH,
        )

    def give(s, direction):
        @pl.when(seg == s)
        def _():
            for conv in (0, 1) if direction == 0 else (1, 0):
                for step in range(1, sections):
                    weight_copy(step, direction, conv).start()

    def pass_on(s, direction, conv):
        step = (seg - s + sections) % sections

        @pl.when(step > 0)
        def _():
            weight_wait(step, direction, conv).wait_recv()
            forward_copy(step, direction, conv).start()

    def arrived(s, direction, conv):
        step = (seg - s + sections) % sections

        @pl.when(step > 0)
        def _():
            forward_copy(step, direction, conv, 1 - core).wait_recv()

    start_halo(frame, 0, 0)

    loads[1].wait()
    spare = jnp.zeros((channels, across - 3 * channels), jnp.float32)
    eye = jnp.where(
        lax.broadcasted_iota(jnp.int32, (channels, channels), 0)
        == lax.broadcasted_iota(jnp.int32, (channels, channels), 1),
        1.0,
        0.0,
    ).astype(jnp.bfloat16)

    def arrange_straight(conv):
        tall = jnp.concatenate(
            [
                own_ref[conv, 9 * (j // 3) + 3 * dy + j % 3] if dy < 3
                else jnp.zeros((across - 3 * channels, channels), jnp.bfloat16)
                for j in range(9)
                for dy in range(4)
            ],
            0,
        )
        wide = lax.dot_general(
            eye, tall, (((1,), (1,)), ((), ())), preferred_element_type=jnp.float32
        ).astype(jnp.bfloat16)
        for j in range(9):
            wbuf[seg, 0, conv, j] = wide[:, j * across : (j + 1) * across]

    def arrange_turned(conv):
        for j in range(9):
            blocks = [
                own_ref[conv, 26 - (9 * (j // 3) + 3 * dy + j % 3)].astype(jnp.float32)
                for dy in range(3)
            ]
            wbuf[seg, 1, conv, j] = jnp.concatenate(blocks + [spare], 1).astype(jnp.bfloat16)

    arrange_straight(0)
    arrange_straight(1)
    give(0, 0)

    zero_half = jnp.zeros((frame.shape[-2], across), jnp.bfloat16)
    zero_row = jnp.zeros((channels, 2 * across), jnp.bfloat16)
    for group in (frame, hidden, sdelta, fdelta):
        for s in range(group.shape[0]):
            group[s, 0, :, :across] = zero_half
            group[s, planes, :, across:] = zero_half
    for group in (hidden, fdelta):
        for s in range(group.shape[0]):
            for p in range(planes + 1):
                group[s, p, :channels] = zero_row
                group[s, p, (inner + 1) * channels :] = zero_row
    for slot in range(2):
        for conv in range(2):
            for piece in range(28, PIECES):
                part[slot, conv, piece] = jnp.zeros((PIECE_ROWS, across), jnp.bfloat16)
    for conv in range(2):
        arrange_turned(conv)
    loads[2].wait()
    for z in range(planes):
        cot_ref[z] = by_plane(cot_flat, z)

    def build(s, direction, conv):
        into = taps.at[s, direction, conv]
        for dz in range(3):
            for dx in range(3):
                compact = wbuf[s, direction, conv, 3 * dz + dx].astype(jnp.float32)
                wide = jnp.concatenate([compact, jnp.zeros_like(compact)], 1)
                for y in range(inner):
                    moved = wide if y == 0 else pltpu.roll(wide, y * channels, 1)
                    row = (3 * y + dx) * channels
                    into[row : row + channels, dz * 2 * across : (dz + 1) * 2 * across] = (
                        moved.astype(jnp.bfloat16)
                    )

    def convolve(s, direction, conv, group, index, pair, low, high):
        matrix = taps[s, direction, conv, 3 * low * channels : 3 * high * channels, :]
        span = group.shape[-2]
        stacked = group[index, 2 * pair : 2 * pair + 3].reshape(3 * span, 2 * across)
        full = jnp.dot(matrix, stacked, preferred_element_type=jnp.float32)
        full = full.reshape(high - low, 3, channels, 2 * across)
        halves = []
        for half in range(2):
            a, b, c = (
                full[:, dx, :, half * across : (half + 1) * across].reshape(
                    (high - low) * channels, across
                )
                for dx in range(3)
            )
            halves.append(shifted(a, 1) + b + shifted(c, -1))
        return halves

    frame_row = lax.broadcasted_iota(jnp.int32, (inner * channels, across), 0) // channels + 1
    inside_low = jnp.where(gy == 0, HALO, 0)
    inside_high = jnp.where(gy == count - 1, rows + HALO, rows + 2 * HALO)
    mask = (frame_row >= inside_low) & (frame_row < inside_high)

    def weight_terms(slot, conv, group, s, delta_group, index):
        for z in range(planes):
            delta = delta_group[index, z + 1, top:bottom, :across].astype(jnp.float32)
            for dx, field in enumerate((shifted(delta, -1), delta, shifted(delta, 1))):
                shifts[
                    z // 2,
                    dx * rows * channels : (dx + 1) * rows * channels,
                    (z % 2) * across : (z % 2 + 1) * across,
                ] = field.astype(jnp.bfloat16)
        lane = lax.broadcasted_iota(jnp.int32, (channels, across), 1) // channels
        fields = []
        for dz in range(3):
            total = None
            for pair in range(planes // 2):
                term = lax.dot_general(
                    group[s, 2 * pair + dz, channels : (inner + 1) * channels, :],
                    shifts[pair],
                    (((1,), (1,)), ((), ())),
                    preferred_element_type=jnp.float32,
                )
                total = term if total is None else total + term
            for dy in range(3):
                for dx in range(3):
                    picked = None
                    for y in range(rows):
                        block = total[
                            (y + dy) * channels : (y + dy + 1) * channels,
                            dx * rows * channels : (dx + 1) * rows * channels,
                        ]
                        picked = block if picked is None else jnp.where(lane == y, block, picked)
                    fields.append(picked)
        fields.append(jnp.zeros((channels, across), jnp.float32))
        first_half = lane < 2
        even = lane % 2 == 0
        half = across // 2
        for k in range(7):
            r = fields[4 * k : 4 * k + 4]
            pairs = [
                jnp.where(first_half, r[i], r[i + 2])
                + pltpu.roll(jnp.where(first_half, r[i + 2], r[i]), half, 1)
                for i in range(2)
            ]
            packed = jnp.where(
                even,
                pairs[0] + pltpu.roll(pairs[0], across - channels, 1),
                pairs[1] + pltpu.roll(pairs[1], channels, 1),
            ).astype(jnp.bfloat16)
            for piece in range(4):
                part[slot, conv, 4 * k + piece] = packed[
                    piece * PIECE_ROWS : (piece + 1) * PIECE_ROWS
                ]

    def out_copy(source, into, kind):
        return pltpu.make_async_remote_copy(
            src_ref=source.at[partner],
            dst_ref=into.at[micro],
            send_sem=out_send.at[kind],
            recv_sem=out_recv.at[kind],
            device_id=(partner, gy),
            device_id_type=MESH,
        )

    me = micro * count + gy
    peers = [(gy + d) % count for d in range(1, count)]

    def share_copy(slot, conv, peer, source=None):
        source = me if source is None else source
        return pltpu.make_async_remote_copy(
            src_ref=part.at[slot, conv, pl.ds(peer * share, share)],
            dst_ref=gathered.at[conv, source],
            send_sem=rs_send.at[conv, slot * count + peer],
            recv_sem=rs_recv.at[conv, source],
            device_id=(2 * upper + slot, peer),
            device_id_type=MESH,
        )

    def send_shares(slot, conv):
        for peer in peers:
            share_copy(slot, conv, peer).start()

        @pl.when(micro != slot)
        def _():
            share_copy(slot, conv, gy).start()

    def whole_copy(conv, peer, owner):
        where = reduced.at[conv, pl.ds(owner * share, share)]
        return pltpu.make_async_remote_copy(
            src_ref=where,
            dst_ref=where,
            send_sem=ag_send.at[conv, peer],
            recv_sem=ag_recv.at[conv, owner],
            device_id=(seg, peer),
            device_id_type=MESH,
        )

    def collect(conv):
        total = part[micro, conv, pl.ds(gy * share, share)].astype(jnp.float32)
        senders = [(1 - micro) * count + gy]
        for peer in peers:
            senders += [peer, count + peer]
        for sender in senders:
            share_copy(1 - micro, conv, gy, sender).wait_recv()
            total = total + gathered[conv, sender].astype(jnp.float32)
        reduced[conv, pl.ds(gy * share, share)] = total.astype(jnp.bfloat16)
        for peer in peers:
            whole_copy(conv, peer, gy).start()

    give(1, 0)
    for conv in range(2):
        pass_on(0, 0, conv)
    for conv in range(2):
        arrived(0, 0, conv)
        build(0, 0, conv)
    for s in range(sections):
        finish_halo(frame, s, s)
        for pair in range(planes // 2):
            for half, pre in enumerate(convolve(s, 0, 0, frame, s, pair, 0, inner)):
                z = 2 * pair + half
                logistic = logistic_of(pre)
                slope1[s, z] = logistic * (1.0 + pre * (1.0 - logistic))
                put(
                    hidden, s, z, channels,
                    jnp.where(mask, pre * logistic, 0.0).astype(jnp.bfloat16),
                )
        for pair in range(planes // 2):
            for half, pre in enumerate(convolve(s, 0, 1, hidden, s, pair, 1, rows + 1)):
                z = 2 * pair + half
                logistic = logistic_of(pre)
                slope = logistic * (1.0 + pre * (1.0 - logistic))
                leaving = (pre * logistic).astype(jnp.bfloat16)
                feats[s, z] = leaving
                if s + 1 == sections:
                    second = (cot_ref[z].astype(jnp.float32) * slope).astype(jnp.bfloat16)
                    put(sdelta, s, z, top, second)
                    continue
                slope2[s, z] = slope
                if s in (1, 2):
                    skip = feats[0, z] if s == 1 else crop_ref[z]
                    leaving = (
                        leaving.astype(jnp.float32) + skip.astype(jnp.float32)
                    ).astype(jnp.bfloat16)
                put(frame, s + 1, z, top, leaving)
        if s + 1 < sections:
            start_halo(frame, s + 1, s + 1)
            if s + 2 < sections:
                give(s + 2, 0)
            give(sections - 1 - s, 1)
            for conv in range(2):
                pass_on(s + 1, 0, conv)
            for conv in range(2):
                arrived(s + 1, 0, conv)
                build(s + 1, 0, conv)
        else:
            start_halo(sdelta, s, sections + s)
            give(0, 1)
            for conv in (1, 0):
                pass_on(s, 1, conv)

    out_copy(feats, feat_out, 0).start()
    feat_out[micro] = feats[seg]
    for conv in (1, 0):
        arrived(sections - 1, 1, conv)
        build(sections - 1, 1, conv)
    for s in reversed(range(sections)):
        @pl.when(upper == s // 2)
        def _():
            weight_terms(s % 2, 1, hidden, s, sdelta, s)
            send_shares(s % 2, 1)

        if s > 0:
            for conv in (1, 0):
                pass_on(s - 1, 1, conv)

        finish_halo(sdelta, s, sections + s)
        for pair in range(planes // 2):
            for half, pre in enumerate(convolve(s, 1, 1, sdelta, s, pair, 0, inner)):
                z = 2 * pair + half
                put(
                    fdelta, 0, z, channels,
                    jnp.where(mask, pre * slope1[s, z], 0.0).astype(jnp.bfloat16),
                )
        if s == 0:
            @pl.when(upper == 0)
            def _():
                weight_terms(0, 0, frame, 0, fdelta, 0)
                send_shares(0, 0)

            collect(1)
        for pair in range(planes // 2):
            for half, pre in enumerate(convolve(s, 1, 0, fdelta, 0, pair, 1, rows + 1)):
                z = 2 * pair + half
                value = pre.astype(jnp.bfloat16)
                if s < 2:
                    value = (
                        value.astype(jnp.float32) + grads[3 - s, z].astype(jnp.float32)
                    ).astype(jnp.bfloat16)
                grads[s, z] = value
                if s > 0:
                    put(
                        sdelta, s - 1, z, top,
                        (value.astype(jnp.float32) * slope2[s - 1, z]).astype(jnp.bfloat16),
                    )
        if s > 0:
            start_halo(sdelta, s - 1, sections + s - 1)
        else:
            out_copy(grads, grad_out, 1).start()
        if s > 0:
            @pl.when(upper == s // 2)
            def _():
                weight_terms(s % 2, 0, frame, s, fdelta, 0)
                send_shares(s % 2, 0)

            for conv in (1, 0):
                arrived(s - 1, 1, conv)
                build(s - 1, 1, conv)

    grad_out[micro] = grads[seg]
    collect(0)
    for conv in (1, 0):
        for peer in peers:
            whole_copy(conv, peer, peer).wait_recv()

    for kind, (source, into) in enumerate(((feats, feat_out), (grads, grad_out))):
        out_copy(source, into, kind).wait()
    for s in range(sections):
        drain_halo(frame, s, s)
        drain_halo(sdelta, s, sections + s)
    for direction in range(2):
        for conv in range(2):
            for step in range(1, sections):
                weight_copy(step, direction, conv).wait_send()
                forward_copy(step, direction, conv).wait_send()
    for conv in range(2):
        for slot in range(2):
            for peer in peers:
                share_copy(slot, conv, peer).wait_send()
        share_copy(1 - micro, conv, gy).wait_send()
        for peer in peers:
            whole_copy(conv, peer, gy).wait_send()


def layout_kernel(
    sizes, feats, grads, reduced, feat_hbm, grad_hbm, wg_hbm, feat_flat, grad_flat, wg_wide, sems
):
    channels, planes, rows, across = sizes
    cells = channels * planes * rows
    place = lax.broadcasted_iota(jnp.int32, (cells, cells), 0)
    source = lax.broadcasted_iota(jnp.int32, (cells, cells), 1)
    wanted = (place % (planes * rows)) * channels + place // (planes * rows)
    pick = jnp.where(source == wanted, 1.0, 0.0).astype(jnp.bfloat16)
    copies = []
    everything = reduced[...].reshape(2, PIECES, PIECE_ROWS, across)
    for conv in range(2):
        for k in range(7):
            block = jnp.concatenate(
                [everything[conv, 4 * k + piece].astype(jnp.float32) for piece in range(4)], 0
            )
            for lane_group in range(4 if k < 6 else 3):
                moved = (
                    pltpu.roll(block, across - lane_group * channels, 1) if lane_group else block
                )
                wg_wide[conv, 4 * k + lane_group] = moved[:, :channels]
        copies.append(pltpu.make_async_copy(wg_wide.at[conv], wg_hbm.at[conv], sems.at[0, conv]))
        copies[-1].start()
    for k, (value, flat, hbm) in enumerate(
        ((grads, grad_flat, grad_hbm), (feats, feat_flat, feat_hbm))
    ):
        for m in range(2):
            flat[m] = jnp.dot(
                pick, value[m].reshape(cells, across), preferred_element_type=jnp.float32
            ).astype(flat.dtype)
            copies.append(pltpu.make_async_copy(flat.at[m], hbm.at[m], sems.at[k + 1, m]))
            copies[-1].start()
    for copy in copies:
        copy.wait()


def local(crops, cotangent, weights):
    micro_count, channels, planes, rows, across = crops.shape
    sizes = (channels, planes, rows, across)
    segment = lax.axis_index("segment")
    sections = lax.axis_size("segment")
    count = lax.axis_size("gy")
    micro = segment % 2
    inner = rows + 2
    span = (rows + 2 * HALO) * channels
    vmem = pl.BlockSpec(memory_space=pltpu.VMEM)
    bf = lambda *shape: pltpu.VMEM(shape, jnp.bfloat16)
    fl = lambda *shape: pltpu.VMEM(shape, jnp.float32)
    dma = lambda *shape: pltpu.SemaphoreType.DMA(shape)

    band = (planes, rows * channels, across)
    double = (planes + 1, span, 2 * across)
    cells = channels * planes * rows
    pieces = (PIECES, PIECE_ROWS, across)
    anywhere = pl.BlockSpec(memory_space=pl.ANY)
    shape = jax.ShapeDtypeStruct
    features, grads, reduced = pl.pallas_call(
        functools.partial(network_kernel, sizes, sections, count),
        out_shape=(
            shape((2, *band), jnp.bfloat16),
            shape((2, *band), jnp.bfloat16),
            shape((2, *pieces), jnp.bfloat16),
        ),
        in_specs=[anywhere] * 3,
        out_specs=(vmem,) * 3,
        scratch_shapes=[
            bf(cells, across),
            bf(cells, across),
            bf(2, 27, channels, channels),
            bf(*band),
            bf(*band),
            bf(sections, *double),
            bf(sections, *double),
            bf(sections, *double),
            bf(1, *double),
            fl(sections, planes, inner * channels, across),
            fl(sections, *band),
            bf(sections, *band),
            bf(sections, *band),
            bf(2 * sections, 2, planes, HALO * channels, across),
            bf(sections, 2, 2, 9, channels, across),
            bf(sections, 2, 2, 3 * inner * channels, 3 * span),
            bf(planes // 2, 3 * rows * channels, 2 * across),
            bf(2, 2, *pieces),
            bf(2, 2 * count, PIECES // count, PIECE_ROWS, across),
            dma(3),
            dma(2 * sections, 2),
            dma(2 * sections, 2),
            dma(sections - 1, 2, 2),
            dma(sections - 1, 2, 2),
            dma(sections - 1, 2, 2),
            dma(sections - 1, 2, 2),
            dma(2),
            dma(2),
            dma(2, 2 * count),
            dma(2, 2 * count),
            dma(2, count),
            dma(2, count),
        ],
        compiler_params=pltpu.CompilerParams(
            vmem_limit_bytes=48 * 2**20, collective_id=0, has_side_effects=True
        ),
    )(
        crops.reshape(micro_count, cells, across),
        cotangent.reshape(micro_count, cells, across),
        weights[0],
    )
    features, grads, weight_grads = pl.pallas_call(
        functools.partial(layout_kernel, sizes),
        out_shape=(
            shape((2, cells, across), jnp.bfloat16),
            shape((2, cells, across), jnp.float32),
            shape((2, 27, channels, channels), jnp.float32),
        ),
        in_specs=[vmem] * 3,
        out_specs=(anywhere,) * 3,
        scratch_shapes=[
            bf(2, cells, across),
            fl(2, cells, across),
            fl(2, 27, channels, channels),
            dma(3, 2),
        ],
        compiler_params=pltpu.CompilerParams(vmem_limit_bytes=8 * 2**20),
    )(features, grads, reduced)
    volume = (1, 2, channels, planes, rows, across)
    return features.reshape(volume), weight_grads[None], grads.reshape(volume)


def solution(mesh):
    return jax.shard_map(
        local,
        mesh=mesh,
        in_specs=(
            P(None, None, None, "gy", None),
            P(None, None, None, "gy", None),
            P("segment", None, None, None, None),
        ),
        out_specs=(
            P("segment", None, None, None, "gy", None),
            P("segment", None, None, None, None),
            P("segment", None, None, None, "gy", None),
        ),
        check_vma=False,
    )
```

```python
import functools

import jax
import jax.numpy as jnp
from jax import lax
from jax.experimental import pallas as pl
from jax.experimental.pallas import tpu as pltpu
from jax.sharding import PartitionSpec as P

HALO = 2
PIECES = 32
PIECE_ROWS = 8
MESH = pl.DeviceIdType.MESH


def logistic_of(value):
    return 0.5 + 0.5 * jnp.tanh(0.5 * value)


def shifted(value, by):
    across = value.shape[-1]
    lane = lax.broadcasted_iota(jnp.int32, value.shape, value.ndim - 1)
    if by == 1:
        return jnp.where(lane == 0, 0.0, pltpu.roll(value, 1, value.ndim - 1))
    return jnp.where(lane == across - 1, 0.0, pltpu.roll(value, across - 1, value.ndim - 1))


def network_kernel(
    sizes,
    sections,
    count,
    crop_hbm,
    cot_hbm,
    own_hbm,
    feat_out,
    grad_out,
    reduced,
    flat,
    own_ref,
    crop_ref,
    cot_ref,
    frame,
    hidden,
    sdelta,
    fdelta,
    slope1,
    slope2,
    feats,
    grads,
    halo,
    wpack,
    taps,
    shifts,
    part,
    gathered,
    in_sem,
    know,
    halo_send,
    halo_recv,
    w_send,
    w_recv,
    f_send,
    f_recv,
    out_send,
    out_recv,
    rs_send,
    rs_recv,
    ag_send,
    ag_recv,
):
    channels, planes, rows, across = sizes
    inner = rows + 2
    seg = lax.axis_index("segment")
    gy = lax.axis_index("gy")
    micro = seg % 2
    upper = seg // 2
    core = gy % 2
    sibling = gy + 1 - 2 * core
    partner = seg + 1 - 2 * micro
    top, bottom = HALO * channels, (HALO + rows) * channels
    share = PIECES // count

    loads = [
        pltpu.make_async_copy(source, into, in_sem.at[k])
        for k, (source, into) in enumerate(
            (
                (own_hbm, own_ref),
                (crop_hbm.at[micro], flat.at[:, pl.ds(0, across)]),
                (cot_hbm.at[micro], flat.at[:, pl.ds(across, across)]),
            )
        )
    ]
    for load in loads:
        load.start()

    def blank(side):
        halo[:, side] = jnp.zeros(halo.shape[:1] + halo.shape[2:], jnp.bfloat16)

    pl.when(gy == 0)(lambda: blank(0))
    pl.when(gy == count - 1)(lambda: blank(1))

    barrier = pltpu.get_barrier_semaphore()

    def greet(s, g):
        pl.semaphore_signal(barrier, inc=1, device_id=(s, g), device_id_type=MESH)

    beside = count <= 2 * sections
    if beside:
        for by in (-1, 1):
            @pl.when((gy + by >= 0) & (gy + by < count))
            def _(by=by):
                greet(seg, gy + by)
                greet(partner, gy + by)

        greet(partner, gy)
        arrivals = 2 * (jnp.where(gy > 0, 1, 0) + jnp.where(gy < count - 1, 1, 0)) + 3
    else:
        for d in range(1, count):
            greet(seg, (gy + d) % count)
        for d in range(count):
            greet(partner, (gy + d) % count)
        arrivals = 2 * count - 1 + 2
    greet((seg + 2) % sections, gy)
    greet((partner + 2) % sections, gy)

    def neighbours():
        return jnp.where(gy > 0, 1, 0) + jnp.where(gy < count - 1, 1, 0)

    rounds = list(range(count - 2)) if beside else []

    def tell():
        if len(told) > len(heard):
            heard.append(told[-1])
            pl.semaphore_wait(know.at[heard[-1]], neighbours())
        if len(told) < len(rounds):
            told.append(len(told))
            for by in (-1, 1):
                @pl.when((gy + by >= 0) & (gy + by < count))
                def _(by=by):
                    pl.semaphore_signal(
                        know.at[told[-1]], inc=1, device_id=(seg, gy + by), device_id_type=MESH
                    )

    told, heard = [], []

    def put(group, s, z, low, value):
        at = pl.ds(low, value.shape[0])
        group[s, z + 1, at, :across] = value
        group[s, z, at, across:] = value

    zero_half = jnp.zeros((frame.shape[-2], across), jnp.bfloat16)
    zero_rows = jnp.zeros((HALO * channels, 2 * across), jnp.bfloat16)
    for group in (frame, hidden, sdelta, fdelta):
        for s in range(group.shape[0]):
            group[s, 0, :, :across] = zero_half
            group[s, planes, :, across:] = zero_half
    for group in (frame, hidden, sdelta, fdelta):
        for s in range(group.shape[0]):
            for p in range(planes + 1):
                group[s, p, :top] = zero_rows
                group[s, p, bottom:] = zero_rows
    for slot in range(2):
        for conv in range(2):
            for piece in range(28, PIECES):
                part[slot, conv, piece] = jnp.zeros((PIECE_ROWS, across), jnp.bfloat16)
    loads[0].wait()
    nothing = jnp.zeros((channels, channels), jnp.float32)
    for conv in range(2):
        for k in range(7):
            wpack[seg, conv, k] = jnp.concatenate(
                [
                    own_ref[conv, 4 * k + g].astype(jnp.float32) if 4 * k + g < 27 else nothing
                    for g in range(4)
                ],
                1,
            ).astype(jnp.bfloat16)

    for load in loads[1:]:
        load.wait()
    size = (rows * channels, channels * planes * rows)
    place = lax.broadcasted_iota(jnp.int32, size, 0)
    origin = (place % channels) * (planes * rows) + place // channels
    source = lax.broadcasted_iota(jnp.int32, size, 1)
    for z in range(planes):
        pick = jnp.where(source == origin + z * rows, 1.0, 0.0).astype(jnp.bfloat16)
        plane = jnp.dot(pick, flat[...], preferred_element_type=jnp.float32).astype(jnp.bfloat16)
        crop_ref[z] = plane[:, :across]
        cot_ref[z] = plane[:, across:]
        put(frame, 0, z, top, plane[:, :across])

    pl.semaphore_wait(barrier, arrivals)

    near, far = 1 - core, core
    deep = HALO * channels

    def halo_copy(group, s, stage, half, pair):
        return pltpu.make_async_remote_copy(
            src_ref=group.at[
                s, pl.ds(2 * pair + 1, 2), pl.ds(pl.multiple_of(top + half * deep, deep), deep),
                pl.ds(0, across),
            ],
            dst_ref=halo.at[stage, 1 - half, pl.ds(2 * pair, 2)],
            send_sem=halo_send.at[stage, half, pair],
            recv_sem=halo_recv.at[stage, 1 - half, pair],
            device_id=(seg, gy - 1 + 2 * half),
            device_id_type=MESH,
        )

    def there(half):
        return (gy - 1 + 2 * half >= 0) & (gy - 1 + 2 * half < count)

    def start_halo(group, s, stage, half, pair):
        @pl.when(there(half))
        def _():
            halo_copy(group, s, stage, half, pair).start()

    def finish_halo(group, s, stage, half):
        @pl.when(there(half))
        def _():
            for pair in range(planes // 2):
                halo_copy(group, s, stage, 1 - half, pair).wait_recv()

        low = pl.multiple_of(half * bottom, channels)
        for z in range(planes):
            put(group, s, z, low, halo[stage, half, z])

    def drain_halo(group, s, stage):
        for half in range(2):
            @pl.when(there(half))
            def _(half=half):
                for pair in range(planes // 2):
                    halo_copy(group, s, stage, half, pair).wait_send()

    half_rows = channels // 2

    def half_of(section, conv, half):
        return wpack.at[section, conv, :, pl.ds(half * half_rows, half_rows)]

    def weight_copy(step, conv, section):
        return pltpu.make_async_remote_copy(
            src_ref=half_of(section, conv, core),
            dst_ref=half_of(section, conv, core),
            send_sem=w_send.at[step - 1, conv],
            recv_sem=w_recv.at[step - 1, conv],
            device_id=((seg + step) % sections, gy),
            device_id_type=MESH,
        )

    def forward_copy(step, conv, half):
        where = half_of((seg - step + sections) % sections, conv, half)
        return pltpu.make_async_remote_copy(
            src_ref=where,
            dst_ref=where,
            send_sem=f_send.at[step - 1, conv],
            recv_sem=f_recv.at[step - 1, conv],
            device_id=(seg, sibling),
            device_id_type=MESH,
        )

    def first_copy(step, conv):
        return pltpu.make_async_remote_copy(
            src_ref=wpack.at[0, conv],
            dst_ref=wpack.at[0, conv],
            send_sem=w_send.at[step - 1, conv],
            recv_sem=w_recv.at[step - 1, conv],
            device_id=((seg + step) % sections, gy),
            device_id_type=MESH,
        )

    def give(s):
        @pl.when(seg == s)
        def _():
            for conv in range(2):
                for step in range(1, sections):
                    if s == 0:
                        first_copy(step, conv).start()
                    else:
                        weight_copy(step, conv, s).start()

    def pass_on(s, conv):
        step = (seg - s + sections) % sections

        @pl.when(step > 0)
        def _():
            weight_copy(step, conv, s).wait_recv()
            forward_copy(step, conv, core).start()

    def arrived(s, conv):
        step = (seg - s + sections) % sections
        if s == 0:
            pl.when(step > 0)(lambda: first_copy(step, conv).wait_recv())
            return

        @pl.when(step > 0)
        def _():
            forward_copy(step, conv, 1 - core).wait_recv()

    give(0)
    for half in (far, near):
        for pair in range(planes // 2):
            start_halo(frame, 0, 0, half, pair)
    give(1)

    lane_group = lax.broadcasted_iota(jnp.int32, (channels, across), 1) // channels
    fold = jnp.where(
        lax.broadcasted_iota(jnp.int32, (channels, across), 0)
        == lax.broadcasted_iota(jnp.int32, (channels, across), 1) % channels,
        1.0,
        0.0,
    ).astype(jnp.bfloat16)

    def compacts(s, direction, conv):
        if direction == 0:
            blocks = []
            for j in range(9):
                for dy in range(4):
                    tap = 9 * (j // 3) + 3 * dy + j % 3
                    blocks.append(
                        jnp.where(
                            lane_group == tap % 4, wpack[s, conv, tap // 4].astype(jnp.float32), 0.0
                        ).astype(jnp.bfloat16)
                        if dy < 3
                        else jnp.zeros((channels, across), jnp.bfloat16)
                    )
            wide = lax.dot_general(
                fold, jnp.concatenate(blocks, 0), (((1,), (1,)), ((), ())),
                preferred_element_type=jnp.float32,
            )
            return [wide[:, j * across : (j + 1) * across] for j in range(9)]
        found = []
        for j in range(9):
            row = jnp.zeros((channels, across), jnp.float32)
            for dy in range(3):
                tap = 26 - (9 * (j // 3) + 3 * dy + j % 3)
                block = wpack[s, conv, tap // 4].astype(jnp.float32)
                by = (dy - tap % 4) % 4
                moved = pltpu.roll(block, by * channels, 1) if by else block
                row = jnp.where(lane_group == dy, moved, row)
            found.append(row)
        return found

    def build(s, direction, conv):
        into = taps.at[s, direction, conv]
        for j, compact in enumerate(compacts(s, direction, conv)):
            dz, dx = j // 3, j % 3
            wide = jnp.concatenate([compact, jnp.zeros_like(compact)], 1)
            for y in range(inner):
                moved = wide if y == 0 else pltpu.roll(wide, y * channels, 1)
                row = (3 * y + dx) * channels
                into[row : row + channels, dz * 2 * across : (dz + 1) * 2 * across] = (
                    moved.astype(jnp.bfloat16)
                )

    def convolve(s, direction, conv, group, index, pair, start):
        at = pl.ds(pl.multiple_of(start * (3 * channels), 3 * channels), 2 * 3 * channels)
        matrix = taps[s, direction, conv, at, :]
        span = group.shape[-2]
        stacked = group[index, 2 * pair : 2 * pair + 3].reshape(3 * span, 2 * across)
        full = jnp.dot(matrix, stacked, preferred_element_type=jnp.float32)
        full = full.reshape(2, 3, channels, 2 * across)
        halves = []
        for half in range(2):
            a, b, c = (
                full[:, dx, :, half * across : (half + 1) * across].reshape(2 * channels, across)
                for dx in range(3)
            )
            halves.append(shifted(a, 1) + b + shifted(c, -1))
        return halves

    inside_low = jnp.where(gy == 0, HALO, 0)
    inside_high = jnp.where(gy == count - 1, rows + HALO, rows + 2 * HALO)
    row_of = lax.broadcasted_iota(jnp.int32, (2 * channels, across), 0) // channels

    def inside(start):
        at = row_of + (start + 1)
        return (at >= inside_low) & (at < inside_high)

    def weight_terms(slot, conv, group, s, delta_group, index):
        for z in range(planes):
            delta = delta_group[index, z + 1, top:bottom, :across].astype(jnp.float32)
            for dx, field in enumerate((shifted(delta, -1), delta, shifted(delta, 1))):
                shifts[
                    dx * rows * channels : (dx + 1) * rows * channels,
                    z * across : (z + 1) * across,
                ] = field.astype(jnp.bfloat16)
        lane = lane_group
        fields = []
        for dz in range(3):
            total = lax.dot_general(
                jnp.concatenate(
                    [
                        group[s, z + dz, channels : (inner + 1) * channels, :]
                        for z in range(0, planes, 2)
                    ],
                    1,
                ),
                shifts[...],
                (((1,), (1,)), ((), ())),
                preferred_element_type=jnp.float32,
            )
            for dy in range(3):
                for dx in range(3):
                    picked = None
                    for y in range(rows):
                        block = total[
                            (y + dy) * channels : (y + dy + 1) * channels,
                            dx * rows * channels : (dx + 1) * rows * channels,
                        ]
                        picked = block if picked is None else jnp.where(lane == y, block, picked)
                    fields.append(picked)
        fields.append(jnp.zeros((channels, across), jnp.float32))
        first_half = lane < 2
        even = lane % 2 == 0
        half = across // 2
        for k in range(7):
            r = fields[4 * k : 4 * k + 4]
            pairs = [
                jnp.where(first_half, r[i], r[i + 2])
                + pltpu.roll(jnp.where(first_half, r[i + 2], r[i]), half, 1)
                for i in range(2)
            ]
            packed = jnp.where(
                even,
                pairs[0] + pltpu.roll(pairs[0], across - channels, 1),
                pairs[1] + pltpu.roll(pairs[1], channels, 1),
            ).astype(jnp.bfloat16)
            for piece in range(4):
                part[slot, conv, 4 * k + piece] = packed[
                    piece * PIECE_ROWS : (piece + 1) * PIECE_ROWS
                ]

    def out_copy(source, into, kind):
        return pltpu.make_async_remote_copy(
            src_ref=source.at[partner],
            dst_ref=into.at[micro],
            send_sem=out_send.at[kind],
            recv_sem=out_recv.at[kind],
            device_id=(partner, gy),
            device_id_type=MESH,
        )

    me = micro * count + gy
    peers = [(gy + d) % count for d in range(1, count)]

    def share_copy(slot, conv, peer, source=None):
        source = me if source is None else source
        return pltpu.make_async_remote_copy(
            src_ref=part.at[slot, conv, pl.ds(peer * share, share)],
            dst_ref=gathered.at[conv, source],
            send_sem=rs_send.at[conv, slot * count + peer],
            recv_sem=rs_recv.at[conv, source],
            device_id=(2 * upper + slot, peer),
            device_id_type=MESH,
        )

    def send_shares(slot, conv):
        for peer in peers:
            share_copy(slot, conv, peer).start()

        @pl.when(micro != slot)
        def _():
            share_copy(slot, conv, gy).start()

    def whole_copy(conv, peer, owner):
        where = reduced.at[conv, pl.ds(owner * share, share)]
        return pltpu.make_async_remote_copy(
            src_ref=where,
            dst_ref=where,
            send_sem=ag_send.at[conv, peer],
            recv_sem=ag_recv.at[conv, owner],
            device_id=(seg, peer),
            device_id_type=MESH,
        )

    def collect(conv):
        total = part[micro, conv, pl.ds(gy * share, share)].astype(jnp.float32)
        senders = [(1 - micro) * count + gy]
        for peer in peers:
            senders += [peer, count + peer]
        for sender in senders:
            share_copy(1 - micro, conv, gy, sender).wait_recv()
            total = total + gathered[conv, sender].astype(jnp.float32)
        reduced[conv, pl.ds(gy * share, share)] = total.astype(jnp.bfloat16)
        for peer in peers:
            whole_copy(conv, peer, gy).start()

    def rows_at(start):
        return pl.ds(pl.multiple_of(start * channels, channels), 2 * channels)

    def forward_first(s, start):
        mask = inside(start)
        for pair in range(planes // 2):
            for half, pre in enumerate(convolve(s, 0, 0, frame, s, pair, start)):
                z = 2 * pair + half
                logistic = logistic_of(pre)
                put(
                    hidden, s, z, pl.multiple_of((start + 1) * channels, channels),
                    jnp.where(mask, pre * logistic, 0.0).astype(jnp.bfloat16),
                )
                slope1[s, z, rows_at(start)] = logistic * (1.0 + pre * (1.0 - logistic))

    def forward_second(s, side):
        at = rows_at(2 * side)
        low = pl.multiple_of(top + side * deep, deep)
        for pair in range(planes // 2):
            for half, pre in enumerate(convolve(s, 0, 1, hidden, s, pair, 1 + 2 * side)):
                z = 2 * pair + half
                logistic = logistic_of(pre)
                slope = logistic * (1.0 + pre * (1.0 - logistic))
                leaving = (pre * logistic).astype(jnp.bfloat16)
                feats[s, z, at] = leaving
                if s + 1 == sections:
                    second = (cot_ref[z, at].astype(jnp.float32) * slope).astype(jnp.bfloat16)
                    put(sdelta, s, z, low, second)
                    continue
                slope2[s, z, at] = slope
                if s in (1, 2):
                    skip = feats[0, z, at] if s == 1 else crop_ref[z, at]
                    leaving = (
                        leaving.astype(jnp.float32) + skip.astype(jnp.float32)
                    ).astype(jnp.bfloat16)
                put(frame, s + 1, z, low, leaving)
            if s + 1 == sections:
                start_halo(sdelta, s, sections + s, side, pair)
            else:
                start_halo(frame, s + 1, s + 1, side, pair)

    def backward_first(s, start):
        mask = inside(start)
        for pair in range(planes // 2):
            for half, pre in enumerate(convolve(s, 1, 1, sdelta, s, pair, start)):
                z = 2 * pair + half
                put(
                    fdelta, s % 2, z, pl.multiple_of((start + 1) * channels, channels),
                    jnp.where(mask, pre * slope1[s, z, rows_at(start)], 0.0).astype(jnp.bfloat16),
                )

    def backward_second(s, side):
        at = rows_at(2 * side)
        low = pl.multiple_of(top + side * deep, deep)
        for pair in range(planes // 2):
            for half, pre in enumerate(convolve(s, 1, 0, fdelta, s % 2, pair, 1 + 2 * side)):
                z = 2 * pair + half
                value = pre.astype(jnp.bfloat16)
                if s < 2:
                    value = (
                        value.astype(jnp.float32) + grads[3 - s, z, at].astype(jnp.float32)
                    ).astype(jnp.bfloat16)
                grads[s, z, at] = value
                if s > 0:
                    put(
                        sdelta, s - 1, z, low,
                        (value.astype(jnp.float32) * slope2[s - 1, z, at]).astype(jnp.bfloat16),
                    )
            if s > 0:
                start_halo(sdelta, s - 1, sections + s - 1, side, pair)

    for s in range(sections):
        if s + 1 < sections and s > 0:
            for conv in range(2):
                pass_on(s + 1, conv)
        arrived(s, 0)
        build(s, 0, 0)
        forward_first(s, 2)
        finish_halo(frame, s, s, near)
        forward_first(s, 4 * near)
        arrived(s, 1)
        build(s, 0, 1)
        if s == 0:
            for later in range(2, sections):
                give(later)
        forward_second(s, near)
        if s > 0:
            tell()
        finish_halo(frame, s, s, far)
        forward_first(s, 4 * far)
        if s == 0:
            for conv in range(2):
                pass_on(1, conv)
        forward_second(s, far)
        tell()

    out_copy(feats, feat_out, 0).start()
    feat_out[micro] = feats[seg]
    for s in reversed(range(sections)):
        build(s, 1, 1)
        backward_first(s, 2)
        finish_halo(sdelta, s, sections + s, near)
        backward_first(s, 4 * near)
        build(s, 1, 0)
        backward_second(s, near)
        if s + 1 < sections:
            @pl.when(upper == (s + 1) // 2)
            def _():
                weight_terms((s + 1) % 2, 0, frame, s + 1, fdelta, (s + 1) % 2)
                send_shares((s + 1) % 2, 0)

        @pl.when(upper == s // 2)
        def _():
            weight_terms(s % 2, 1, hidden, s, sdelta, s)
            send_shares(s % 2, 1)

        finish_halo(sdelta, s, sections + s, far)
        backward_first(s, 4 * far)
        if s == 0:
            @pl.when(upper == 0)
            def _():
                weight_terms(0, 0, frame, 0, fdelta, 0)
                send_shares(0, 0)

        backward_second(s, far)

        @pl.when(partner == s)
        def _():
            out_copy(grads, grad_out, 1).start()

    collect(1)
    grad_out[micro] = grads[seg]
    collect(0)
    for conv in (1, 0):
        for peer in peers:
            whole_copy(conv, peer, peer).wait_recv()

    for kind, (source, into) in enumerate(((feats, feat_out), (grads, grad_out))):
        out_copy(source, into, kind).wait()
    for s in range(sections):
        drain_halo(frame, s, s)
        drain_halo(sdelta, s, sections + s)
    for conv in range(2):
        for step in range(1, sections):
            @pl.when(seg == 0)
            def _():
                first_copy(step, conv).wait_send()

            @pl.when(seg > 0)
            def _():
                weight_copy(step, conv, seg).wait_send()

            @pl.when(seg != step)
            def _():
                forward_copy(step, conv, core).wait_send()
    for conv in range(2):
        for slot in range(2):
            for peer in peers:
                share_copy(slot, conv, peer).wait_send()
        share_copy(1 - micro, conv, gy).wait_send()
        for peer in peers:
            whole_copy(conv, peer, gy).wait_send()


def layout_kernel(
    sizes, feats, grads, reduced, feat_hbm, grad_hbm, wg_hbm, feat_flat, grad_flat, wg_wide, sems
):
    channels, planes, rows, across = sizes
    cells = channels * planes * rows
    place = lax.broadcasted_iota(jnp.int32, (cells, cells), 0)
    source = lax.broadcasted_iota(jnp.int32, (cells, cells), 1)
    wanted = (place % (planes * rows)) * channels + place // (planes * rows)
    pick = jnp.where(source == wanted, 1.0, 0.0).astype(jnp.bfloat16)
    copies = []
    everything = reduced[...].reshape(2, PIECES, PIECE_ROWS, across)
    for conv in range(2):
        for k in range(7):
            block = jnp.concatenate(
                [everything[conv, 4 * k + piece].astype(jnp.float32) for piece in range(4)], 0
            )
            for lane_group in range(4 if k < 6 else 3):
                moved = (
                    pltpu.roll(block, across - lane_group * channels, 1) if lane_group else block
                )
                wg_wide[conv, 4 * k + lane_group] = moved[:, :channels]
        copies.append(pltpu.make_async_copy(wg_wide.at[conv], wg_hbm.at[conv], sems.at[0, conv]))
        copies[-1].start()
    for k, (value, flat, hbm) in enumerate(
        ((grads, grad_flat, grad_hbm), (feats, feat_flat, feat_hbm))
    ):
        for m in range(2):
            flat[m] = jnp.dot(
                pick, value[m].reshape(cells, across), preferred_element_type=jnp.float32
            ).astype(flat.dtype)
            copies.append(pltpu.make_async_copy(flat.at[m], hbm.at[m], sems.at[k + 1, m]))
            copies[-1].start()
    for copy in copies:
        copy.wait()


def local(crops, cotangent, weights):
    micro_count, channels, planes, rows, across = crops.shape
    sizes = (channels, planes, rows, across)
    segment = lax.axis_index("segment")
    sections = lax.axis_size("segment")
    count = lax.axis_size("gy")
    micro = segment % 2
    inner = rows + 2
    span = (rows + 2 * HALO) * channels
    vmem = pl.BlockSpec(memory_space=pltpu.VMEM)
    bf = lambda *shape: pltpu.VMEM(shape, jnp.bfloat16)
    fl = lambda *shape: pltpu.VMEM(shape, jnp.float32)
    dma = lambda *shape: pltpu.SemaphoreType.DMA(shape)

    band = (planes, rows * channels, across)
    double = (planes + 1, span, 2 * across)
    cells = channels * planes * rows
    pieces = (PIECES, PIECE_ROWS, across)
    anywhere = pl.BlockSpec(memory_space=pltpu.HBM)
    shape = jax.ShapeDtypeStruct
    features, grads, reduced = pl.pallas_call(
        functools.partial(network_kernel, sizes, sections, count),
        out_shape=(
            shape((2, *band), jnp.bfloat16),
            shape((2, *band), jnp.bfloat16),
            shape((2, *pieces), jnp.bfloat16),
        ),
        in_specs=[anywhere] * 3,
        out_specs=(vmem,) * 3,
        scratch_shapes=[
            bf(cells, 2 * across),
            bf(2, 27, channels, channels),
            bf(*band),
            bf(*band),
            bf(sections, *double),
            bf(sections, *double),
            bf(sections, *double),
            bf(2, *double),
            fl(sections, planes, inner * channels, across),
            fl(sections, *band),
            bf(sections, *band),
            bf(sections, *band),
            bf(2 * sections, 2, planes, HALO * channels, across),
            bf(sections, 2, 7, channels, across),
            bf(sections, 2, 2, 3 * inner * channels, 3 * span),
            bf(3 * rows * channels, planes * across),
            bf(2, 2, *pieces),
            bf(2, 2 * count, PIECES // count, PIECE_ROWS, across),
            dma(3),
            pltpu.SemaphoreType.REGULAR((2 * sections,)),
            dma(2 * sections, 2, planes // 2),
            dma(2 * sections, 2, planes // 2),
            dma(sections - 1, 2),
            dma(sections - 1, 2),
            dma(sections - 1, 2),
            dma(sections - 1, 2),
            dma(2),
            dma(2),
            dma(2, 2 * count),
            dma(2, 2 * count),
            dma(2, count),
            dma(2, count),
        ],
        compiler_params=pltpu.CompilerParams(
            vmem_limit_bytes=48 * 2**20, collective_id=0, has_side_effects=True
        ),
    )(
        crops.reshape(micro_count, cells, across),
        cotangent.reshape(micro_count, cells, across),
        weights[0],
    )
    features, grads, weight_grads = pl.pallas_call(
        functools.partial(layout_kernel, sizes),
        out_shape=(
            shape((2, cells, across), jnp.bfloat16),
            shape((2, cells, across), jnp.float32),
            shape((2, 27, channels, channels), jnp.float32),
        ),
        in_specs=[vmem] * 3,
        out_specs=(anywhere,) * 3,
        scratch_shapes=[
            bf(2, cells, across),
            fl(2, cells, across),
            fl(2, 27, channels, channels),
            dma(3, 2),
        ],
        compiler_params=pltpu.CompilerParams(vmem_limit_bytes=8 * 2**20),
    )(features, grads, reduced)
    volume = (1, 2, channels, planes, rows, across)
    return features.reshape(volume), weight_grads[None], grads.reshape(volume)


def solution(mesh):
    return jax.shard_map(
        local,
        mesh=mesh,
        in_specs=(
            P(None, None, None, "gy", None),
            P(None, None, None, "gy", None),
            P("segment", None, None, None, None),
        ),
        out_specs=(
            P("segment", None, None, None, "gy", None),
            P("segment", None, None, None, None),
            P("segment", None, None, None, "gy", None),
        ),
        check_vma=False,
    )
```

```python
import functools

import jax
import jax.numpy as jnp
from jax import lax
from jax.experimental import pallas as pl
from jax.experimental.pallas import tpu as pltpu
from jax.sharding import PartitionSpec as P

HALO = 2
PIECES = 32
PIECE_ROWS = 8
MESH = pl.DeviceIdType.MESH


def logistic_of(value):
    return 0.5 + 0.5 * jnp.tanh(0.5 * value)


def shifted(value, by):
    across = value.shape[-1]
    lane = lax.broadcasted_iota(jnp.int32, value.shape, value.ndim - 1)
    if by == 1:
        return jnp.where(lane == 0, 0.0, pltpu.roll(value, 1, value.ndim - 1))
    return jnp.where(lane == across - 1, 0.0, pltpu.roll(value, across - 1, value.ndim - 1))


def network_kernel(
    sizes,
    sections,
    count,
    crop_hbm,
    cot_hbm,
    own_hbm,
    feat_out,
    grad_out,
    reduced,
    flat,
    own_ref,
    crop_ref,
    cot_ref,
    frame,
    hidden,
    sdelta,
    fdelta,
    slope1,
    slope2,
    feats,
    grads,
    halo,
    wpack,
    taps,
    shifts,
    part,
    gathered,
    in_sem,
    know,
    halo_send,
    halo_recv,
    w_send,
    w_recv,
    f_send,
    f_recv,
    out_send,
    out_recv,
    rs_send,
    rs_recv,
    ag_send,
    ag_recv,
):
    channels, planes, rows, across = sizes
    inner = rows + 2
    seg = lax.axis_index("segment")
    gy = lax.axis_index("gy")
    micro = seg % 2
    upper = seg // 2
    core = gy % 2
    sibling = gy + 1 - 2 * core
    partner = seg + 1 - 2 * micro
    top, bottom = HALO * channels, (HALO + rows) * channels
    share = PIECES // count

    loads = [
        pltpu.make_async_copy(source, into, in_sem.at[k])
        for k, (source, into) in enumerate(
            (
                (own_hbm, own_ref),
                (crop_hbm.at[micro], flat.at[:, pl.ds(0, across)]),
                (cot_hbm.at[micro], flat.at[:, pl.ds(across, across)]),
            )
        )
    ]
    for load in loads:
        load.start()

    def blank(side):
        halo[:, side] = jnp.zeros(halo.shape[:1] + halo.shape[2:], jnp.bfloat16)

    pl.when(gy == 0)(lambda: blank(0))
    pl.when(gy == count - 1)(lambda: blank(1))

    barrier = pltpu.get_barrier_semaphore()

    def greet(s, g):
        pl.semaphore_signal(barrier, inc=1, device_id=(s, g), device_id_type=MESH)

    beside = count <= 2 * sections
    if beside:
        for by in (-1, 1):
            @pl.when((gy + by >= 0) & (gy + by < count))
            def _(by=by):
                greet(seg, gy + by)
                greet(partner, gy + by)

        greet(partner, gy)
        arrivals = 2 * (jnp.where(gy > 0, 1, 0) + jnp.where(gy < count - 1, 1, 0)) + 3
    else:
        for d in range(1, count):
            greet(seg, (gy + d) % count)
        for d in range(count):
            greet(partner, (gy + d) % count)
        arrivals = 2 * count - 1 + 2
    greet((seg + 2) % sections, gy)
    greet((partner + 2) % sections, gy)

    def neighbours():
        return jnp.where(gy > 0, 1, 0) + jnp.where(gy < count - 1, 1, 0)

    rounds = list(range(count - 2)) if beside else []

    def tell():
        if len(told) > len(heard):
            heard.append(told[-1])
            pl.semaphore_wait(know.at[heard[-1]], neighbours())
        if len(told) < len(rounds):
            told.append(len(told))
            for by in (-1, 1):
                @pl.when((gy + by >= 0) & (gy + by < count))
                def _(by=by):
                    pl.semaphore_signal(
                        know.at[told[-1]], inc=1, device_id=(seg, gy + by), device_id_type=MESH
                    )

    told, heard = [], []

    def put(group, s, z, low, value):
        at = pl.ds(low, value.shape[0])
        group[s, z + 1, at, :across] = value
        group[s, z, at, across:] = value

    zero_half = jnp.zeros((frame.shape[-2], across), jnp.bfloat16)
    zero_rows = jnp.zeros((HALO * channels, 2 * across), jnp.bfloat16)
    for group in (frame, hidden, sdelta, fdelta):
        for s in range(group.shape[0]):
            group[s, 0, :, :across] = zero_half
            group[s, planes, :, across:] = zero_half
    for group in (frame, hidden, sdelta, fdelta):
        for s in range(group.shape[0]):
            for p in range(planes + 1):
                group[s, p, :top] = zero_rows
                group[s, p, bottom:] = zero_rows
    for slot in range(2):
        for conv in range(2):
            for piece in range(28, PIECES):
                part[slot, conv, piece] = jnp.zeros((PIECE_ROWS, across), jnp.bfloat16)
    loads[0].wait()
    nothing = jnp.zeros((channels, channels), jnp.float32)
    for conv in range(2):
        for k in range(7):
            wpack[seg, conv, k] = jnp.concatenate(
                [
                    own_ref[conv, 4 * k + g].astype(jnp.float32) if 4 * k + g < 27 else nothing
                    for g in range(4)
                ],
                1,
            ).astype(jnp.bfloat16)

    for load in loads[1:]:
        load.wait()
    size = (rows * channels, channels * planes * rows)
    place = lax.broadcasted_iota(jnp.int32, size, 0)
    origin = (place % channels) * (planes * rows) + place // channels
    source = lax.broadcasted_iota(jnp.int32, size, 1)
    for z in range(planes):
        pick = jnp.where(source == origin + z * rows, 1.0, 0.0).astype(jnp.bfloat16)
        plane = jnp.dot(pick, flat[...], preferred_element_type=jnp.float32).astype(jnp.bfloat16)
        crop_ref[z] = plane[:, :across]
        cot_ref[z] = plane[:, across:]
        put(frame, 0, z, top, plane[:, :across])

    pl.semaphore_wait(barrier, arrivals)

    near, far = 1 - core, core
    deep = HALO * channels

    def halo_copy(group, s, stage, half, pair):
        return pltpu.make_async_remote_copy(
            src_ref=group.at[
                s, pl.ds(2 * pair + 1, 2), pl.ds(pl.multiple_of(top + half * deep, deep), deep),
                pl.ds(0, across),
            ],
            dst_ref=halo.at[stage, 1 - half, pl.ds(2 * pair, 2)],
            send_sem=halo_send.at[stage, half, pair],
            recv_sem=halo_recv.at[stage, 1 - half, pair],
            device_id=(seg, gy - 1 + 2 * half),
            device_id_type=MESH,
        )

    def there(half):
        return (gy - 1 + 2 * half >= 0) & (gy - 1 + 2 * half < count)

    def start_halo(group, s, stage, half, pair):
        @pl.when(there(half))
        def _():
            halo_copy(group, s, stage, half, pair).start()

    def finish_halo(group, s, stage, half):
        @pl.when(there(half))
        def _():
            for pair in range(planes // 2):
                halo_copy(group, s, stage, 1 - half, pair).wait_recv()

        low = pl.multiple_of(half * bottom, channels)
        for z in range(planes):
            put(group, s, z, low, halo[stage, half, z])

    def drain_halo(group, s, stage):
        for half in range(2):
            @pl.when(there(half))
            def _(half=half):
                for pair in range(planes // 2):
                    halo_copy(group, s, stage, half, pair).wait_send()

    half_rows = channels // 2

    def half_of(section, conv, half):
        return wpack.at[section, conv, :, pl.ds(half * half_rows, half_rows)]

    def weight_copy(step, conv, section):
        return pltpu.make_async_remote_copy(
            src_ref=half_of(section, conv, core),
            dst_ref=half_of(section, conv, core),
            send_sem=w_send.at[step - 1, conv],
            recv_sem=w_recv.at[step - 1, conv],
            device_id=((seg + step) % sections, gy),
            device_id_type=MESH,
        )

    def forward_copy(step, conv, half):
        where = half_of((seg - step + sections) % sections, conv, half)
        return pltpu.make_async_remote_copy(
            src_ref=where,
            dst_ref=where,
            send_sem=f_send.at[step - 1, conv],
            recv_sem=f_recv.at[step - 1, conv],
            device_id=(seg, sibling),
            device_id_type=MESH,
        )

    def first_copy(step, conv):
        return pltpu.make_async_remote_copy(
            src_ref=wpack.at[0, conv],
            dst_ref=wpack.at[0, conv],
            send_sem=w_send.at[step - 1, conv],
            recv_sem=w_recv.at[step - 1, conv],
            device_id=((seg + step) % sections, gy),
            device_id_type=MESH,
        )

    def give(s):
        @pl.when(seg == s)
        def _():
            for conv in range(2):
                for step in range(1, sections):
                    if s == 0:
                        first_copy(step, conv).start()
                    else:
                        weight_copy(step, conv, s).start()

    def pass_on(s, conv):
        step = (seg - s + sections) % sections

        @pl.when(step > 0)
        def _():
            weight_copy(step, conv, s).wait_recv()
            forward_copy(step, conv, core).start()

    def arrived(s, conv):
        step = (seg - s + sections) % sections
        if s == 0:
            pl.when(step > 0)(lambda: first_copy(step, conv).wait_recv())
            return

        @pl.when(step > 0)
        def _():
            forward_copy(step, conv, 1 - core).wait_recv()

    give(0)
    for half in (far, near):
        for pair in range(planes // 2):
            start_halo(frame, 0, 0, half, pair)
    give(1)

    lane_group = lax.broadcasted_iota(jnp.int32, (channels, across), 1) // channels
    fold = jnp.where(
        lax.broadcasted_iota(jnp.int32, (channels, across), 0)
        == lax.broadcasted_iota(jnp.int32, (channels, across), 1) % channels,
        1.0,
        0.0,
    ).astype(jnp.bfloat16)

    def compacts(s, direction, conv):
        if direction == 0:
            blocks = []
            for j in range(9):
                for dy in range(4):
                    tap = 9 * (j // 3) + 3 * dy + j % 3
                    blocks.append(
                        jnp.where(
                            lane_group == tap % 4, wpack[s, conv, tap // 4].astype(jnp.float32), 0.0
                        ).astype(jnp.bfloat16)
                        if dy < 3
                        else jnp.zeros((channels, across), jnp.bfloat16)
                    )
            wide = lax.dot_general(
                fold, jnp.concatenate(blocks, 0), (((1,), (1,)), ((), ())),
                preferred_element_type=jnp.float32,
            )
            return [wide[:, j * across : (j + 1) * across] for j in range(9)]
        found = []
        for j in range(9):
            row = jnp.zeros((channels, across), jnp.float32)
            for dy in range(3):
                tap = 26 - (9 * (j // 3) + 3 * dy + j % 3)
                block = wpack[s, conv, tap // 4].astype(jnp.float32)
                by = (dy - tap % 4) % 4
                moved = pltpu.roll(block, by * channels, 1) if by else block
                row = jnp.where(lane_group == dy, moved, row)
            found.append(row)
        return found

    def build(s, direction, conv):
        into = taps.at[s, direction, conv]
        for j, compact in enumerate(compacts(s, direction, conv)):
            dz, dx = j // 3, j % 3
            wide = jnp.concatenate([compact, jnp.zeros_like(compact)], 1)
            for y in range(inner):
                moved = wide if y == 0 else pltpu.roll(wide, y * channels, 1)
                row = (3 * y + dx) * channels
                into[row : row + channels, dz * 2 * across : (dz + 1) * 2 * across] = (
                    moved.astype(jnp.bfloat16)
                )

    def convolve(s, direction, conv, group, index, pair, start):
        at = pl.ds(pl.multiple_of(start * (3 * channels), 3 * channels), 2 * 3 * channels)
        matrix = taps[s, direction, conv, at, :]
        span = group.shape[-2]
        stacked = group[index, 2 * pair : 2 * pair + 3].reshape(3 * span, 2 * across)
        full = jnp.dot(matrix, stacked, preferred_element_type=jnp.float32)
        full = full.reshape(2, 3, channels, 2 * across)
        halves = []
        for half in range(2):
            a, b, c = (
                full[:, dx, :, half * across : (half + 1) * across].reshape(2 * channels, across)
                for dx in range(3)
            )
            halves.append(shifted(a, 1) + b + shifted(c, -1))
        return halves

    inside_low = jnp.where(gy == 0, HALO, 0)
    inside_high = jnp.where(gy == count - 1, rows + HALO, rows + 2 * HALO)
    row_of = lax.broadcasted_iota(jnp.int32, (2 * channels, across), 0) // channels

    def inside(start):
        at = row_of + (start + 1)
        return (at >= inside_low) & (at < inside_high)

    def weight_terms(slot, conv, group, s, delta_group, index):
        for z in range(planes):
            delta = delta_group[index, z + 1, top:bottom, :across].astype(jnp.float32)
            for dx, field in enumerate((shifted(delta, -1), delta, shifted(delta, 1))):
                shifts[
                    dx * rows * channels : (dx + 1) * rows * channels,
                    z * across : (z + 1) * across,
                ] = field.astype(jnp.bfloat16)
        lane = lane_group
        fields = []
        for dz in range(3):
            total = lax.dot_general(
                jnp.concatenate(
                    [
                        group[s, z + dz, channels : (inner + 1) * channels, :]
                        for z in range(0, planes, 2)
                    ],
                    1,
                ),
                shifts[...],
                (((1,), (1,)), ((), ())),
                preferred_element_type=jnp.float32,
            )
            for dy in range(3):
                for dx in range(3):
                    picked = None
                    for y in range(rows):
                        block = total[
                            (y + dy) * channels : (y + dy + 1) * channels,
                            dx * rows * channels : (dx + 1) * rows * channels,
                        ]
                        picked = block if picked is None else jnp.where(lane == y, block, picked)
                    fields.append(picked)
        fields.append(jnp.zeros((channels, across), jnp.float32))
        first_half = lane < 2
        even = lane % 2 == 0
        half = across // 2
        for k in range(7):
            r = fields[4 * k : 4 * k + 4]
            pairs = [
                jnp.where(first_half, r[i], r[i + 2])
                + pltpu.roll(jnp.where(first_half, r[i + 2], r[i]), half, 1)
                for i in range(2)
            ]
            packed = jnp.where(
                even,
                pairs[0] + pltpu.roll(pairs[0], across - channels, 1),
                pairs[1] + pltpu.roll(pairs[1], channels, 1),
            ).astype(jnp.bfloat16)
            for piece in range(4):
                part[slot, conv, 4 * k + piece] = packed[
                    piece * PIECE_ROWS : (piece + 1) * PIECE_ROWS
                ]

    def out_copy(source, into, kind):
        return pltpu.make_async_remote_copy(
            src_ref=source.at[partner],
            dst_ref=into.at[micro],
            send_sem=out_send.at[kind],
            recv_sem=out_recv.at[kind],
            device_id=(partner, gy),
            device_id_type=MESH,
        )

    me = micro * count + gy
    peers = [(gy + d) % count for d in range(1, count)]

    def share_copy(slot, conv, peer, source=None):
        source = me if source is None else source
        return pltpu.make_async_remote_copy(
            src_ref=part.at[slot, conv, pl.ds(peer * share, share)],
            dst_ref=gathered.at[conv, source],
            send_sem=rs_send.at[conv, slot * count + peer],
            recv_sem=rs_recv.at[conv, source],
            device_id=(2 * upper + slot, peer),
            device_id_type=MESH,
        )

    def send_shares(slot, conv):
        for peer in peers:
            share_copy(slot, conv, peer).start()

        @pl.when(micro != slot)
        def _():
            share_copy(slot, conv, gy).start()

    def whole_copy(conv, peer, owner):
        where = reduced.at[conv, pl.ds(owner * share, share)]
        return pltpu.make_async_remote_copy(
            src_ref=where,
            dst_ref=where,
            send_sem=ag_send.at[conv, peer],
            recv_sem=ag_recv.at[conv, owner],
            device_id=(seg, peer),
            device_id_type=MESH,
        )

    def collect(conv):
        total = part[micro, conv, pl.ds(gy * share, share)].astype(jnp.float32)
        senders = [(1 - micro) * count + gy]
        for peer in peers:
            senders += [peer, count + peer]
        for sender in senders:
            share_copy(1 - micro, conv, gy, sender).wait_recv()
            total = total + gathered[conv, sender].astype(jnp.float32)
        reduced[conv, pl.ds(gy * share, share)] = total.astype(jnp.bfloat16)
        for peer in peers:
            whole_copy(conv, peer, gy).start()

    def rows_at(start):
        return pl.ds(pl.multiple_of(start * channels, channels), 2 * channels)

    def forward_first(s, start):
        mask = inside(start)
        for pair in range(planes // 2):
            for half, pre in enumerate(convolve(s, 0, 0, frame, s, pair, start)):
                z = 2 * pair + half
                logistic = logistic_of(pre)
                put(
                    hidden, s, z, pl.multiple_of((start + 1) * channels, channels),
                    jnp.where(mask, pre * logistic, 0.0).astype(jnp.bfloat16),
                )
                slope1[s, z, rows_at(start)] = logistic * (1.0 + pre * (1.0 - logistic))

    def forward_second(s, side):
        at = rows_at(2 * side)
        low = pl.multiple_of(top + side * deep, deep)
        for pair in range(planes // 2):
            for half, pre in enumerate(convolve(s, 0, 1, hidden, s, pair, 1 + 2 * side)):
                z = 2 * pair + half
                logistic = logistic_of(pre)
                slope = logistic * (1.0 + pre * (1.0 - logistic))
                leaving = (pre * logistic).astype(jnp.bfloat16)
                feats[s, z, at] = leaving
                if s + 1 == sections:
                    second = (cot_ref[z, at].astype(jnp.float32) * slope).astype(jnp.bfloat16)
                    put(sdelta, s, z, low, second)
                    continue
                slope2[s, z, at] = slope
                if s in (1, 2):
                    skip = feats[0, z, at] if s == 1 else crop_ref[z, at]
                    leaving = (
                        leaving.astype(jnp.float32) + skip.astype(jnp.float32)
                    ).astype(jnp.bfloat16)
                put(frame, s + 1, z, low, leaving)
            if s + 1 == sections:
                start_halo(sdelta, s, sections + s, side, pair)
            else:
                start_halo(frame, s + 1, s + 1, side, pair)

    def backward_first(s, start):
        mask = inside(start)
        for pair in range(planes // 2):
            for half, pre in enumerate(convolve(s, 1, 1, sdelta, s, pair, start)):
                z = 2 * pair + half
                put(
                    fdelta, s % 2, z, pl.multiple_of((start + 1) * channels, channels),
                    jnp.where(mask, pre * slope1[s, z, rows_at(start)], 0.0).astype(jnp.bfloat16),
                )

    def backward_second(s, side):
        at = rows_at(2 * side)
        low = pl.multiple_of(top + side * deep, deep)
        for pair in range(planes // 2):
            for half, pre in enumerate(convolve(s, 1, 0, fdelta, s % 2, pair, 1 + 2 * side)):
                z = 2 * pair + half
                value = pre.astype(jnp.bfloat16)
                if s < 2:
                    value = (
                        value.astype(jnp.float32) + grads[3 - s, z, at].astype(jnp.float32)
                    ).astype(jnp.bfloat16)
                grads[s, z, at] = value
                if s > 0:
                    put(
                        sdelta, s - 1, z, low,
                        (value.astype(jnp.float32) * slope2[s - 1, z, at]).astype(jnp.bfloat16),
                    )
            if s > 0:
                start_halo(sdelta, s - 1, sections + s - 1, side, pair)

    for s in range(sections):
        if s + 1 < sections and s > 0:
            for conv in range(2):
                pass_on(s + 1, conv)
        arrived(s, 0)
        build(s, 0, 0)
        forward_first(s, 2)
        finish_halo(frame, s, s, near)
        forward_first(s, 4 * near)
        arrived(s, 1)
        build(s, 0, 1)
        if s == 0:
            for later in range(2, sections):
                give(later)
        forward_second(s, near)
        if s > 0:
            tell()
        finish_halo(frame, s, s, far)
        forward_first(s, 4 * far)
        if s == 0:
            for conv in range(2):
                pass_on(1, conv)
        forward_second(s, far)
        tell()

    out_copy(feats, feat_out, 0).start()
    feat_out[micro] = feats[seg]
    for s in reversed(range(sections)):
        build(s, 1, 1)
        backward_first(s, 2)
        finish_halo(sdelta, s, sections + s, near)
        backward_first(s, 4 * near)
        build(s, 1, 0)
        backward_second(s, near)
        if s + 1 < sections:
            @pl.when(upper == (s + 1) // 2)
            def _():
                weight_terms((s + 1) % 2, 0, frame, s + 1, fdelta, (s + 1) % 2)
                send_shares((s + 1) % 2, 0)

        @pl.when(upper == s // 2)
        def _():
            weight_terms(s % 2, 1, hidden, s, sdelta, s)
            send_shares(s % 2, 1)

        finish_halo(sdelta, s, sections + s, far)
        backward_first(s, 4 * far)
        if s == 0:
            @pl.when(upper == 0)
            def _():
                weight_terms(0, 0, frame, 0, fdelta, 0)
                send_shares(0, 0)

        backward_second(s, far)

        @pl.when(partner == s)
        def _():
            out_copy(grads, grad_out, 1).start()

    collect(1)
    grad_out[micro] = grads[seg]
    collect(0)
    for conv in (1, 0):
        for peer in peers:
            whole_copy(conv, peer, peer).wait_recv()

    for kind, (source, into) in enumerate(((feats, feat_out), (grads, grad_out))):
        out_copy(source, into, kind).wait()
    for s in range(sections):
        drain_halo(frame, s, s)
        drain_halo(sdelta, s, sections + s)
    for conv in range(2):
        for step in range(1, sections):
            @pl.when(seg == 0)
            def _():
                first_copy(step, conv).wait_send()

            @pl.when(seg > 0)
            def _():
                weight_copy(step, conv, seg).wait_send()

            @pl.when(seg != step)
            def _():
                forward_copy(step, conv, core).wait_send()
    for conv in range(2):
        for slot in range(2):
            for peer in peers:
                share_copy(slot, conv, peer).wait_send()
        share_copy(1 - micro, conv, gy).wait_send()
        for peer in peers:
            whole_copy(conv, peer, gy).wait_send()


def layout_kernel(
    sizes, feats, grads, reduced, feat_hbm, grad_hbm, wg_hbm, feat_flat, grad_flat, wg_wide, sems
):
    channels, planes, rows, across = sizes
    cells = channels * planes * rows
    place = lax.broadcasted_iota(jnp.int32, (cells, cells), 0)
    source = lax.broadcasted_iota(jnp.int32, (cells, cells), 1)
    wanted = (place % (planes * rows)) * channels + place // (planes * rows)
    pick = jnp.where(source == wanted, 1.0, 0.0).astype(jnp.bfloat16)
    copies = []
    everything = reduced[...].reshape(2, PIECES, PIECE_ROWS, across)
    for conv in range(2):
        for k in range(7):
            block = jnp.concatenate(
                [everything[conv, 4 * k + piece].astype(jnp.float32) for piece in range(4)], 0
            )
            for lane_group in range(4 if k < 6 else 3):
                moved = (
                    pltpu.roll(block, across - lane_group * channels, 1) if lane_group else block
                )
                wg_wide[conv, 4 * k + lane_group] = moved[:, :channels]
        copies.append(pltpu.make_async_copy(wg_wide.at[conv], wg_hbm.at[conv], sems.at[0, conv]))
        copies[-1].start()
    for k, (value, flat, hbm) in enumerate(
        ((grads, grad_flat, grad_hbm), (feats, feat_flat, feat_hbm))
    ):
        for m in range(2):
            flat[m] = jnp.dot(
                pick, value[m].reshape(cells, across), preferred_element_type=jnp.float32
            ).astype(flat.dtype)
            copies.append(pltpu.make_async_copy(flat.at[m], hbm.at[m], sems.at[k + 1, m]))
            copies[-1].start()
    for copy in copies:
        copy.wait()


def local(crops, cotangent, weights):
    micro_count, channels, planes, rows, across = crops.shape
    sizes = (channels, planes, rows, across)
    segment = lax.axis_index("segment")
    sections = lax.axis_size("segment")
    count = lax.axis_size("gy")
    micro = segment % 2
    inner = rows + 2
    span = (rows + 2 * HALO) * channels
    vmem = pl.BlockSpec(memory_space=pltpu.VMEM)
    bf = lambda *shape: pltpu.VMEM(shape, jnp.bfloat16)
    fl = lambda *shape: pltpu.VMEM(shape, jnp.float32)
    dma = lambda *shape: pltpu.SemaphoreType.DMA(shape)

    band = (planes, rows * channels, across)
    double = (planes + 1, span, 2 * across)
    cells = channels * planes * rows
    pieces = (PIECES, PIECE_ROWS, across)
    anywhere = pl.BlockSpec(memory_space=pltpu.HBM)
    shape = jax.ShapeDtypeStruct
    features, grads, reduced = pl.pallas_call(
        functools.partial(network_kernel, sizes, sections, count),
        out_shape=(
            shape((2, *band), jnp.bfloat16),
            shape((2, *band), jnp.bfloat16),
            shape((2, *pieces), jnp.bfloat16),
        ),
        in_specs=[anywhere] * 3,
        out_specs=(vmem,) * 3,
        scratch_shapes=[
            bf(cells, 2 * across),
            bf(2, 27, channels, channels),
            bf(*band),
            bf(*band),
            bf(sections, *double),
            bf(sections, *double),
            bf(sections, *double),
            bf(2, *double),
            fl(sections, planes, inner * channels, across),
            fl(sections, *band),
            bf(sections, *band),
            bf(sections, *band),
            bf(2 * sections, 2, planes, HALO * channels, across),
            bf(sections, 2, 7, channels, across),
            bf(sections, 2, 2, 3 * inner * channels, 3 * span),
            bf(3 * rows * channels, planes * across),
            bf(2, 2, *pieces),
            bf(2, 2 * count, PIECES // count, PIECE_ROWS, across),
            dma(3),
            pltpu.SemaphoreType.REGULAR((2 * sections,)),
            dma(2 * sections, 2, planes // 2),
            dma(2 * sections, 2, planes // 2),
            dma(sections - 1, 2),
            dma(sections - 1, 2),
            dma(sections - 1, 2),
            dma(sections - 1, 2),
            dma(2),
            dma(2),
            dma(2, 2 * count),
            dma(2, 2 * count),
            dma(2, count),
            dma(2, count),
        ],
        compiler_params=pltpu.CompilerParams(
            vmem_limit_bytes=48 * 2**20, collective_id=0, has_side_effects=True
        ),
    )(
        pltpu.with_memory_space_constraint(crops.reshape(micro_count, cells, across), pltpu.HBM),
        pltpu.with_memory_space_constraint(cotangent.reshape(micro_count, cells, across), pltpu.HBM),
        pltpu.with_memory_space_constraint(weights[0], pltpu.HBM),
    )
    features, grads, weight_grads = pl.pallas_call(
        functools.partial(layout_kernel, sizes),
        out_shape=(
            shape((2, cells, across), jnp.bfloat16),
            shape((2, cells, across), jnp.float32),
            shape((2, 27, channels, channels), jnp.float32),
        ),
        in_specs=[vmem] * 3,
        out_specs=(anywhere,) * 3,
        scratch_shapes=[
            bf(2, cells, across),
            fl(2, cells, across),
            fl(2, 27, channels, channels),
            dma(3, 2),
        ],
        compiler_params=pltpu.CompilerParams(vmem_limit_bytes=8 * 2**20),
    )(features, grads, reduced)
    volume = (1, 2, channels, planes, rows, across)
    return features.reshape(volume), weight_grads[None], grads.reshape(volume)


def solution(mesh):
    return jax.shard_map(
        local,
        mesh=mesh,
        in_specs=(
            P(None, None, None, "gy", None),
            P(None, None, None, "gy", None),
            P("segment", None, None, None, None),
        ),
        out_specs=(
            P("segment", None, None, None, "gy", None),
            P("segment", None, None, None, None),
            P("segment", None, None, None, "gy", None),
        ),
        check_vma=False,
    )
```
